8 devices in a mesh: pairs: 2 (over z, y), rows: 4 (over x, core).
Axes of the slice: x: 2, y: 2, z: 1, core: 2. Of those that a mesh axis runs over, the one named last changes fastest.
Arguments:
- cost_src: float32 [8192, 4096], P(('pairs', 'rows')), parts along dimension 0
- cost_tgt: float32 [8192, 4096], P(('pairs', 'rows')), parts along dimension 0
- plan_init: float32 [8192, 4096], P(('pairs', 'rows')), parts along dimension 0
- mass_src: float32 [8192], P(('pairs', 'rows')), parts along dimension 0
- mass_tgt: float32 [8192], P('pairs'), parts along dimension 0
- feat_src: float32 [8192, 256], P(('pairs', 'rows')), parts along dimension 0
- feat_tgt: float32 [8192, 256], P(('pairs', 'rows')), parts along dimension 0
- epsilon: float32 [], replicated
Outputs:
- output: float32 [8192, 4096], P(('pairs', 'rows')), parts along dimension 0
There are 2 independent parts. The reference program is written for one: setup_inputs(seed, part) draws one part's arguments, and reference() takes and returns one part's arrays. A program takes and returns all parts, laid end to end along the dimension named above; an argument that names none is the same for every part.
All inputs are finite; a program needn't handle non-finite values.
Results may differ from the reference program's by a relative error of at most 0.001.
Values are sent between devices in bfloat16 or wider.
A program may use at most 1 GiB of HBM per device.

```python
import jax
import jax.numpy as jnp
from jax import lax

N = 4096
M = 4096
D = 256
OUTER_STEPS = 2
SWEEPS = 10
ALPHA = 0.5


def point_costs(key_pts, num_points):
    key_centers, key_labels, key_noise = jax.random.split(key_pts, 3)
    centers = 1.5 * jax.random.normal(key_centers, (8, 3), jnp.float32)
    labels = jax.random.randint(key_labels, (num_points,), 0, 8)
    points = centers[labels] + 0.4 * jax.random.normal(key_noise, (num_points, 3), jnp.float32)
    sq_dist = jnp.zeros((num_points, num_points), jnp.float32)
    for dim_index in range(3):
        column_vals = points[:, dim_index]
        coord_diff = column_vals[:, None] - column_vals[None, :]
        sq_dist = sq_dist + coord_diff * coord_diff
    return sq_dist / jnp.max(sq_dist), labels


def marginal(key_mass, num_points):
    weights = jnp.exp(0.5 * jax.random.normal(key_mass, (num_points,), jnp.float32))
    return weights / jnp.sum(weights)


def setup_inputs(seed: int = 0, part: int = 0) -> dict:
    base_key, shared_key = jax.random.split(jax.random.key(seed))
    sub_keys = jax.random.split(jax.random.fold_in(base_key, part), 7)
    cost_src, labels_src = point_costs(sub_keys[0], N)
    cost_tgt, labels_tgt = point_costs(sub_keys[1], M)
    mass_src = marginal(sub_keys[2], N)
    mass_tgt = marginal(sub_keys[3], M)
    block_logits = 3.0 * jax.random.normal(sub_keys[4], (8, 8), jnp.float32)
    plan_init = mass_src[:, None] * mass_tgt[None, :] * jnp.exp(block_logits[labels_src][:, labels_tgt])
    plan_init = plan_init / jnp.sum(plan_init)
    feat_scale = 0.125 * D ** -0.25
    feat_src = feat_scale * jax.random.normal(sub_keys[5], (N, D), jnp.float32)
    feat_tgt = feat_scale * jax.random.normal(sub_keys[6], (M, D), jnp.float32)
    epsilon = jax.random.uniform(shared_key, (), jnp.float32, 0.04, 0.08)
    return {"cost_src": cost_src, "cost_tgt": cost_tgt, "plan_init": plan_init, "mass_src": mass_src, "mass_tgt": mass_tgt, "feat_src": feat_src, "feat_tgt": feat_tgt, "epsilon": epsilon}


def reference(cost_src, cost_tgt, plan_init, mass_src, mass_tgt, feat_src, feat_tgt, epsilon):
    src_half = cost_src.astype(jnp.bfloat16)
    tgt_half = cost_tgt.astype(jnp.bfloat16)
    cross_term = jnp.dot(feat_src.astype(jnp.bfloat16), feat_tgt.astype(jnp.bfloat16).T, preferred_element_type=jnp.float32)
    feat_cost = (-2.0 * ALPHA) * cross_term

    def outer_step(step_index, transport):
        prod_a = jnp.dot(src_half, transport.astype(jnp.bfloat16), preferred_element_type=jnp.float32)
        prod_b = jnp.dot(prod_a.astype(jnp.bfloat16), tgt_half, preferred_element_type=jnp.float32)
        step_cost = feat_cost - (2.0 * (1.0 - ALPHA)) * prod_b
        kernel = jnp.exp(-(step_cost - jnp.min(step_cost, axis=1, keepdims=True)) / epsilon)

        def sinkhorn_sweep(sweep_index, scales):
            row_scale = mass_src / jnp.sum(kernel * scales[1][None, :], axis=1)
            return row_scale, mass_tgt / jnp.sum(kernel * row_scale[:, None], axis=0)

        start_scales = (jnp.ones_like(mass_src), jnp.ones_like(mass_tgt))
        row_scale, col_scale = lax.fori_loop(0, SWEEPS, sinkhorn_sweep, start_scales)
        return row_scale[:, None] * kernel * col_scale[None, :]

    return lax.fori_loop(0, OUTER_STEPS, outer_step, plan_init)
```

```python
import functools

import jax
import jax.numpy as jnp
from jax import lax
from jax.experimental import pallas as pl
from jax.experimental.pallas import tpu as pltpu
from jax.sharding import PartitionSpec as P

ALPHA = 0.5
OUTER_STEPS = 2
SWEEPS = 10
LANES = 128
CHUNKS = 4
BLOCK = 64
LOAD_ROWS = 128
MESH = pl.DeviceIdType.MESH


def sinkhorn_kernel(group, gain_hbm, mass_row, mass_col, epsilon, plan_hbm, kern, plan, row_scale, acc, col_scale,
                    part_sum, peer_sum, load_sem, store_sem, send_sem, recv_sem):
    rows, cols = kern.shape
    tiles = cols // LANES // CHUNKS
    width = cols // CHUNKS
    me = lax.axis_index('rows')
    peers = [lax.rem(me + k, group) for k in range(1, group)]

    loads = [pltpu.make_async_copy(gain_hbm.at[pl.ds(b * LOAD_ROWS, LOAD_ROWS)], kern.at[pl.ds(b * LOAD_ROWS, LOAD_ROWS)],
                                   load_sem.at[b]) for b in range(rows // LOAD_ROWS)]
    for load in loads:
        load.start()

    barrier = pltpu.get_barrier_semaphore()
    for peer in peers:
        pl.semaphore_signal(barrier, inc=1, device_id={'rows': peer}, device_id_type=MESH)
    pl.semaphore_wait(barrier, group - 1)

    def tile(j, t):
        start = j * width + t * LANES
        return slice(start, start + LANES)

    def sends(slot, j):
        return [pltpu.make_async_remote_copy(
            src_ref=part_sum.at[slot, j], dst_ref=peer_sum.at[slot, k, j], send_sem=send_sem.at[slot, k, j],
            recv_sem=recv_sem.at[slot, k, j], device_id={'rows': peers[k]}, device_id_type=MESH) for k in range(group - 1)]

    inv_eps = 1.0 / epsilon[0]
    for b, load in enumerate(loads):
        load.wait()

        def exp_block(i, carry, b=b):
            span = pl.ds(b * LOAD_ROWS + i * BLOCK, BLOCK)
            top = kern[span, 0:LANES]
            for t in range(1, cols // LANES):
                top = jnp.maximum(top, kern[span, t * LANES:(t + 1) * LANES])
            top = jnp.max(top, axis=1, keepdims=True)
            total = jnp.zeros((BLOCK, LANES), jnp.float32)
            for t in range(cols // LANES):
                val = jnp.exp((kern[span, t * LANES:(t + 1) * LANES] - top) * inv_eps)
                kern[span, t * LANES:(t + 1) * LANES] = val
                total = total + val
            acc[span, :] = total
            return carry
        lax.fori_loop(0, LOAD_ROWS // BLOCK, exp_block, 0)

    def row_update():
        for h in range(0, rows, 256):
            span = slice(h, h + 256)
            row_scale[span, :] = mass_row[span, :] / jnp.sum(acc[span, :], axis=1, keepdims=True)

    def col_pass(slot, j):
        def body(i, sums):
            span = pl.ds(i * BLOCK, BLOCK)
            scale = row_scale[span, :].reshape(BLOCK // 8, 8, LANES)
            return tuple(sums[t] + jnp.sum(kern[span, tile(j, t)].reshape(BLOCK // 8, 8, LANES) * scale, axis=0)
                         for t in range(tiles))
        sums = lax.fori_loop(0, rows // BLOCK, body, tuple(jnp.zeros((8, LANES), jnp.float32) for _ in range(tiles)))
        part_sum[slot, j] = jnp.concatenate([jnp.sum(s, axis=0, keepdims=True) for s in sums], axis=0)
        for send in sends(slot, j):
            send.start()

    def col_update(slot, j):
        for send in sends(slot, j):
            send.wait()
        total = part_sum[slot, j]
        for k in range(group - 1):
            total = total + peer_sum[slot, k, j]
        col_scale[j] = mass_col[j] / total

    def scale_rows(j):
        return [jnp.broadcast_to(col_scale[j, t:t + 1, :], (8, LANES)) for t in range(tiles)]

    def row_pass(j):
        scale = scale_rows(j)

        def body(i, carry):
            span = pl.ds(i * BLOCK, BLOCK)
            total = None if j == 0 else acc[span, :].reshape(BLOCK // 8, 8, LANES)
            for t in range(tiles):
                term = kern[span, tile(j, t)].reshape(BLOCK // 8, 8, LANES) * scale[t][None]
                total = term if total is None else total + term
            acc[span, :] = total.reshape(BLOCK, LANES)
            return carry
        lax.fori_loop(0, rows // BLOCK, body, 0)

    row_update()

    def sweep(n, carry):
        slot = lax.rem(n, 2)
        for j in range(CHUNKS):
            col_pass(slot, j)
        for j in range(CHUNKS):
            col_update(slot, j)
            row_pass(j)
        row_update()
        return carry
    lax.fori_loop(0, SWEEPS - 1, sweep, 0)

    last = (SWEEPS - 1) % 2
    for j in range(CHUNKS):
        col_pass(last, j)
    stores = []
    for j in range(CHUNKS):
        col_update(last, j)
        scale = scale_rows(j)

        def plan_block(i, carry, j=j, scale=scale):
            span = pl.ds(i * BLOCK, BLOCK)
            left = row_scale[span, :].reshape(BLOCK // 8, 8, LANES)
            for t in range(tiles):
                val = left * kern[span, tile(j, t)].reshape(BLOCK // 8, 8, LANES) * scale[t][None]
                plan[span, tile(j, t)] = val.reshape(BLOCK, LANES).astype(plan.dtype)
            return carry
        lax.fori_loop(0, rows // BLOCK, plan_block, 0)
        span = pl.ds(j * width, width)
        stores.append(pltpu.make_async_copy(plan.at[:, span], plan_hbm.at[:, span], store_sem.at[j]))
        stores[-1].start()
    for store in stores:
        store.wait()


def sinkhorn(group, gain, mass_rows, mass_tgt, epsilon, dtype, collective_id):
    rows, cols = gain.shape
    tiles = cols // LANES // CHUNKS
    row_rep = jnp.broadcast_to(mass_rows[:, None], (rows, LANES))
    col_tiles = mass_tgt.reshape(CHUNKS, tiles, LANES)
    n_load = rows // LOAD_ROWS
    return pl.pallas_call(
        functools.partial(sinkhorn_kernel, group),
        out_shape=jax.ShapeDtypeStruct((rows, cols), dtype),
        in_specs=[pl.BlockSpec(memory_space=pl.ANY), pl.BlockSpec(memory_space=pltpu.VMEM),
                  pl.BlockSpec(memory_space=pltpu.VMEM), pl.BlockSpec(memory_space=pltpu.SMEM)],
        out_specs=pl.BlockSpec(memory_space=pl.ANY),
        scratch_shapes=[
            pltpu.VMEM((rows, cols), jnp.float32),
            pltpu.VMEM((rows, cols), dtype),
            pltpu.VMEM((rows, LANES), jnp.float32),
            pltpu.VMEM((rows, LANES), jnp.float32),
            pltpu.VMEM((CHUNKS, tiles, LANES), jnp.float32),
            pltpu.VMEM((2, CHUNKS, tiles, LANES), jnp.float32),
            pltpu.VMEM((2, group - 1, CHUNKS, tiles, LANES), jnp.float32),
            pltpu.SemaphoreType.DMA((n_load,)),
            pltpu.SemaphoreType.DMA((CHUNKS,)),
            pltpu.SemaphoreType.DMA((2, group - 1, CHUNKS)),
            pltpu.SemaphoreType.DMA((2, group - 1, CHUNKS)),
        ],
        compiler_params=pltpu.CompilerParams(collective_id=collective_id, has_side_effects=True,
                                             vmem_limit_bytes=48 * 1024 * 1024),
        cost_estimate=pl.CostEstimate(flops=4 * SWEEPS * rows * cols, bytes_accessed=8 * rows * cols,
                                      transcendentals=rows * cols),
        name='sinkhorn',
    )(gain, row_rep, col_tiles, epsilon.reshape(1))


def solution(mesh):
    group = mesh.shape['rows']

    def local_fgw(cost_src, cost_tgt, plan_init, mass_src, mass_tgt, feat_src, feat_tgt, epsilon):
        src_half = cost_src.astype(jnp.bfloat16)
        tgt_half = cost_tgt.astype(jnp.bfloat16)
        feat_all = lax.all_gather(feat_tgt.astype(jnp.bfloat16), 'rows', tiled=True)
        cross_term = jnp.einsum('id,jd->ij', feat_src.astype(jnp.bfloat16), feat_all, preferred_element_type=jnp.float32)
        tgt_all = lax.all_gather(tgt_half, 'rows', tiled=True)
        transport = plan_init.astype(jnp.bfloat16)
        for step_index in range(OUTER_STEPS):
            transport_all = lax.all_gather(transport, 'rows', tiled=True)
            prod_a = jnp.dot(src_half, transport_all, preferred_element_type=jnp.float32)
            prod_b = jnp.dot(prod_a.astype(jnp.bfloat16), tgt_all, preferred_element_type=jnp.float32)
            gain = (2.0 * ALPHA) * cross_term + (2.0 * (1.0 - ALPHA)) * prod_b
            last = step_index == OUTER_STEPS - 1
            transport = sinkhorn(group, gain, mass_src, mass_tgt, epsilon,
                                 jnp.float32 if last else jnp.bfloat16, step_index)
        return transport

    row_spec = P(('pairs', 'rows'), None)
    vec_spec = P(('pairs', 'rows'))
    in_specs = (row_spec, row_spec, row_spec, vec_spec, P('pairs'), row_spec, row_spec, P())
    return jax.shard_map(local_fgw, mesh=mesh, in_specs=in_specs, out_specs=row_spec, check_vma=False)
```

```python
import functools

import jax
import jax.numpy as jnp
from jax import lax
from jax.experimental import pallas as pl
from jax.experimental.pallas import tpu as pltpu
from jax.sharding import PartitionSpec as P

ALPHA = 0.5
SWEEPS = 10
LANES = 128
CHUNKS = 4
BLOCK = 64
LOAD_ROWS = 128
STEP_WIDTHS = (512, 512, 512, 256, 256)
ROW_PARTS = 4
MESH = pl.DeviceIdType.MESH


def sinkhorn_kernel(group, n_gain, transposed, *refs):
    gains, refs = refs[:n_gain], refs[n_gain:]
    (mass_row, mass_col, epsilon, plan_hbm, kern, plan, row_scale, acc, col_scale, shift_fix,
     part_sum, peer_sum, part_top, peer_top, load_sem, store_sem, send_sem, recv_sem, top_send, top_recv) = refs
    rows, cols = kern.shape
    tiles = cols // LANES // CHUNKS
    width = cols // CHUNKS
    gain_rows = rows // n_gain
    me = lax.axis_index('rows')
    chip, core = me // 2, me % 2
    peers = [chip * 2 + (1 - core), (1 - chip) * 2 + core, (1 - chip) * 2 + (1 - core)]

    if transposed:
        loads = [pltpu.make_async_copy(gains[0].at[:, pl.ds(j * width, width)], kern.at[:, pl.ds(j * width, width)],
                                       load_sem.at[j]) for j in range(CHUNKS)]
    else:
        loads = []
        for b in range(rows // LOAD_ROWS):
            start = b * LOAD_ROWS
            source = gains[start // gain_rows].at[pl.ds(start % gain_rows, LOAD_ROWS)]
            loads.append(pltpu.make_async_copy(source, kern.at[pl.ds(start, LOAD_ROWS)], load_sem.at[b]))
    for load in loads:
        load.start()

    barrier = pltpu.get_barrier_semaphore()
    for peer in peers:
        pl.semaphore_signal(barrier, inc=1, device_id={'rows': peer}, device_id_type=MESH)
    pl.semaphore_wait(barrier, group - 1)

    def tile(j, t):
        start = j * width + t * LANES
        return slice(start, start + LANES)

    def sends(slot, j):
        return [pltpu.make_async_remote_copy(
            src_ref=part_sum.at[slot, j], dst_ref=peer_sum.at[slot, k, j], send_sem=send_sem.at[slot, k, j],
            recv_sem=recv_sem.at[slot, k, j], device_id={'rows': peers[k]}, device_id_type=MESH) for k in range(group - 1)]

    def top_sends(j):
        return [pltpu.make_async_remote_copy(
            src_ref=part_top.at[j], dst_ref=peer_top.at[k, j], send_sem=top_send.at[k, j],
            recv_sem=top_recv.at[k, j], device_id={'rows': peers[k]}, device_id_type=MESH) for k in range(group - 1)]

    inv_eps = 1.0 / epsilon[0]

    def split(val):
        return val.reshape(val.shape[0] // 8, 8, LANES)

    def row_update():
        for h in range(0, rows, 256):
            span = slice(h, h + 256)
            row_scale[span, :] = mass_row[span, :] / jnp.sum(acc[span, :], axis=1, keepdims=True)

    def col_pass(slot, j):
        def body(i, sums):
            span = pl.ds(i * BLOCK, BLOCK)
            scale = split(row_scale[span, :])
            return tuple(sums[t] + jnp.sum(split(kern[span, tile(j, t)]) * scale, axis=0) for t in range(tiles))
        sums = lax.fori_loop(0, rows // BLOCK, body, tuple(jnp.zeros((8, LANES), jnp.float32) for _ in range(tiles)))
        total = jnp.concatenate([jnp.sum(s, axis=0, keepdims=True) for s in sums], axis=0)
        if transposed:
            total = total * shift_fix[j]
        part_sum[slot, j] = total
        for send in sends(slot, j):
            send.start()

    def col_update(slot, j):
        for send in sends(slot, j):
            send.wait()
        total = part_sum[slot, j]
        for k in range(group - 1):
            total = total + peer_sum[slot, k, j]
        scale = mass_col[j] / total
        if transposed:
            scale = scale * shift_fix[j]
        col_scale[j] = scale

    def scale_rows(j):
        return [jnp.broadcast_to(col_scale[j, t:t + 1, :], (8, LANES)) for t in range(tiles)]

    def row_pass(j):
        scale = scale_rows(j)

        def body(i, carry):
            span = pl.ds(i * BLOCK, BLOCK)
            total = None if j == 0 else split(acc[span, :])
            for t in range(tiles):
                term = split(kern[span, tile(j, t)]) * scale[t][None]
                total = term if total is None else total + term
            acc[span, :] = total.reshape(BLOCK, LANES)
            return carry
        lax.fori_loop(0, rows // BLOCK, body, 0)

    def plan_chunk(j):
        scale = scale_rows(j)

        def plan_block(i, carry):
            span = pl.ds(i * BLOCK, BLOCK)
            left = split(row_scale[span, :])
            for t in range(tiles):
                val = left * split(kern[span, tile(j, t)]) * scale[t][None]
                plan[span, tile(j, t)] = val.reshape(BLOCK, LANES).astype(plan.dtype)
            return carry
        lax.fori_loop(0, rows // BLOCK, plan_block, 0)
        span = pl.ds(j * width, width)
        store = pltpu.make_async_copy(plan.at[:, span], plan_hbm.at[:, span], store_sem.at[j])
        store.start()
        return store

    if transposed:
        for j in range(CHUNKS):
            loads[j].wait()

            def top_block(i, tops, j=j):
                span = pl.ds(i * BLOCK, BLOCK)
                return tuple(jnp.maximum(tops[t], jnp.max(split(kern[span, tile(j, t)]), axis=0)) for t in range(tiles))
            tops = lax.fori_loop(0, rows // BLOCK, top_block,
                                 tuple(kern[0:8, tile(j, t)] for t in range(tiles)))
            tops = [jnp.max(top, axis=0, keepdims=True) for top in tops]
            wide = [jnp.broadcast_to(top, (8, LANES)) for top in tops]

            def exp_block(i, sums, j=j, wide=wide):
                span = pl.ds(i * BLOCK, BLOCK)
                out = []
                for t in range(tiles):
                    val = jnp.exp((split(kern[span, tile(j, t)]) - wide[t][None]) * inv_eps)
                    kern[span, tile(j, t)] = val.reshape(BLOCK, LANES)
                    out.append(sums[t] + jnp.sum(val, axis=0))
                return tuple(out)
            sums = lax.fori_loop(0, rows // BLOCK, exp_block,
                                 tuple(jnp.zeros((8, LANES), jnp.float32) for _ in range(tiles)))
            part_top[j, 0] = jnp.concatenate(tops, axis=0)
            part_top[j, 1] = jnp.concatenate([jnp.sum(s, axis=0, keepdims=True) for s in sums], axis=0)
            for send in top_sends(j):
                send.start()
        for j in range(CHUNKS):
            for send in top_sends(j):
                send.wait()
            top = part_top[j, 0]
            for k in range(group - 1):
                top = jnp.maximum(top, peer_top[k, j, 0])
            fix = jnp.exp((part_top[j, 0] - top) * inv_eps)
            total = part_top[j, 1] * fix
            for k in range(group - 1):
                total = total + peer_top[k, j, 1] * jnp.exp((peer_top[k, j, 0] - top) * inv_eps)
            shift_fix[j] = fix
            col_scale[j] = mass_col[j] / total * fix
            row_pass(j)
        row_update()
    else:
        for b, load in enumerate(loads):
            load.wait()

            def exp_rows(i, carry, b=b):
                span = pl.ds(b * LOAD_ROWS + i * BLOCK, BLOCK)
                top = kern[span, 0:LANES]
                for t in range(1, cols // LANES):
                    top = jnp.maximum(top, kern[span, t * LANES:(t + 1) * LANES])
                top = jnp.max(top, axis=1, keepdims=True)
                total = jnp.zeros((BLOCK, LANES), jnp.float32)
                for t in range(cols // LANES):
                    val = jnp.exp((kern[span, t * LANES:(t + 1) * LANES] - top) * inv_eps)
                    kern[span, t * LANES:(t + 1) * LANES] = val
                    total = total + val
                acc[span, :] = total
                return carry
            lax.fori_loop(0, LOAD_ROWS // BLOCK, exp_rows, 0)
        row_update()

    def sweep(n, carry):
        slot = lax.rem(n, 2)
        for j in range(CHUNKS):
            col_pass(slot, j)
        for j in range(CHUNKS):
            col_update(slot, j)
            row_pass(j)
        row_update()
        return carry
    lax.fori_loop(0, SWEEPS - 1, sweep, 0)

    stores = []
    if transposed:
        for j in range(CHUNKS):
            stores.append(plan_chunk(j))
    else:
        last = (SWEEPS - 1) % 2
        for j in range(CHUNKS):
            col_pass(last, j)
        for j in range(CHUNKS):
            col_update(last, j)
            stores.append(plan_chunk(j))
    for store in stores:
        store.wait()


def sinkhorn(group, gains, mass_row, mass_col, epsilon, dtype, transposed, collective_id):
    cols = gains[0].shape[1]
    rows = sum(g.shape[0] for g in gains)
    tiles = cols // LANES // CHUNKS
    row_rep = jnp.broadcast_to(mass_row[:, None], (rows, LANES))
    col_tiles = mass_col.reshape(CHUNKS, tiles, LANES)
    n_load = CHUNKS if transposed else rows // LOAD_ROWS
    vec = (CHUNKS, tiles, LANES)
    pair = (CHUNKS, 2, tiles, LANES)
    return pl.pallas_call(
        functools.partial(sinkhorn_kernel, group, len(gains), transposed),
        out_shape=jax.ShapeDtypeStruct((rows, cols), dtype),
        in_specs=[pl.BlockSpec(memory_space=pl.ANY)] * len(gains) + [
            pl.BlockSpec(memory_space=pltpu.VMEM), pl.BlockSpec(memory_space=pltpu.VMEM),
            pl.BlockSpec(memory_space=pltpu.SMEM)],
        out_specs=pl.BlockSpec(memory_space=pl.ANY),
        scratch_shapes=[
            pltpu.VMEM((rows, cols), jnp.float32),
            pltpu.VMEM((rows, cols), dtype),
            pltpu.VMEM((rows, LANES), jnp.float32),
            pltpu.VMEM((rows, LANES), jnp.float32),
            pltpu.VMEM(vec, jnp.float32),
            pltpu.VMEM(vec, jnp.float32),
            pltpu.VMEM((2,) + vec, jnp.float32),
            pltpu.VMEM((2, group - 1) + vec, jnp.float32),
            pltpu.VMEM(pair, jnp.float32),
            pltpu.VMEM((group - 1,) + pair, jnp.float32),
            pltpu.SemaphoreType.DMA((n_load,)),
            pltpu.SemaphoreType.DMA((CHUNKS,)),
            pltpu.SemaphoreType.DMA((2, group - 1, CHUNKS)),
            pltpu.SemaphoreType.DMA((2, group - 1, CHUNKS)),
            pltpu.SemaphoreType.DMA((group - 1, CHUNKS)),
            pltpu.SemaphoreType.DMA((group - 1, CHUNKS)),
        ],
        compiler_params=pltpu.CompilerParams(collective_id=collective_id, has_side_effects=True,
                                             vmem_limit_bytes=48 * 1024 * 1024),
        cost_estimate=pl.CostEstimate(flops=4 * SWEEPS * rows * cols, bytes_accessed=8 * rows * cols,
                                      transcendentals=rows * cols),
        name='sinkhorn_cols' if transposed else 'sinkhorn_rows',
    )(*gains, row_rep, col_tiles, epsilon.reshape(1))


def swap(value, distance):
    return lax.ppermute(value, 'rows', [(i, i ^ distance) for i in range(4)])


class Wire:
    def __init__(self):
        self.landed = []

    def send(self, value, distance):
        if len(self.landed) >= 2:
            value, self.landed[-2] = lax.optimization_barrier((value, self.landed[-2]))
        self.landed.append(swap(value, distance))
        return len(self.landed) - 1

    def get(self, index):
        return self.landed[index]


def solution(mesh):
    group = mesh.shape['rows']

    def local_fgw(cost_src, cost_tgt, plan_init, mass_src, mass_tgt, feat_src, feat_tgt, epsilon):
        rows, cols = cost_src.shape
        half = cols // 2
        quad = rows // 2
        me = lax.axis_index('rows')
        chip, core = me // 2, me % 2
        even = core == 0
        dot = functools.partial(jnp.einsum, preferred_element_type=jnp.float32)
        wire = Wire()

        def ordered(mine, other, axis=0):
            return jnp.where(even, jnp.concatenate([mine, other], axis), jnp.concatenate([other, mine], axis))

        def chip_order(mine, other, axis):
            return jnp.where(chip == 0, jnp.concatenate([mine, other], axis), jnp.concatenate([other, mine], axis))

        def pack(cost):
            diag = lax.dynamic_slice(cost, (0, rows * me), (rows, rows))
            off = lax.dynamic_slice(cost, (0, rows * (me + 1 - 2 * core)), (rows, rows))
            edge = jnp.where(even, off[:quad, :], off[:, quad:].T)
            return jnp.concatenate([diag[:quad, :quad], diag[:quad, quad:], diag[quad:, quad:],
                                    edge[:, :quad], edge[:, quad:]], axis=0)

        def assemble(cost, packed):
            near = ordered(cost, swap(cost, 1))
            packed_pair = swap(packed, 1)
            packs = [jnp.where(even, packed, packed_pair), jnp.where(even, packed_pair, packed)]
            diags, edges = [], []
            for item in packs:
                p = [item[k * quad:(k + 1) * quad] for k in range(5)]
                diags.append(jnp.block([[p[0], p[1]], [p[1].T, p[2]]]))
                edges.append(jnp.concatenate([p[3], p[4]], axis=1))
            edge = jnp.concatenate(edges, axis=0)
            far = jnp.block([[diags[0], edge], [edge.T, diags[1]]])
            turned = lax.dynamic_slice(near, (0, half * (1 - chip)), (half, half)).T
            return jnp.concatenate([near, chip_order(turned, far, 1)], axis=0)

        src_half = cost_src.astype(jnp.bfloat16)
        tgt_half = cost_tgt.astype(jnp.bfloat16)
        feats = jnp.concatenate([feat_src, feat_tgt], axis=1).astype(jnp.bfloat16)
        start = plan_init.astype(jnp.bfloat16)
        depth = feat_src.shape[1]

        src_wire = wire.send(pack(src_half), 2)
        feat_wire = wire.send(feats, 2)
        start_mine = lax.dynamic_slice(start, (0, half * core), (rows, half))
        start_other = lax.dynamic_slice(start, (0, half * (1 - core)), (rows, half))
        spans, at = [], 0
        for w in STEP_WIDTHS:
            spans.append((at, at + w))
            at += w
        plan_wires = []
        for lo, hi in spans:
            plan_wires.append((wire.send(start_mine[:, lo:hi], 2), wire.send(start_other[:, lo:hi], 3)))
        tgt_wire = wire.send(pack(tgt_half), 2)

        src_all = assemble(src_half, wire.get(src_wire))
        feat_near = ordered(feats, swap(feats, 1))
        feat_far = ordered(wire.get(feat_wire), swap(wire.get(feat_wire), 1))
        feat_all = chip_order(feat_near, feat_far, 0)
        start_pair = swap(start_other, 1)
        tgt_mine = lax.dynamic_slice(tgt_half, (0, half * core), (rows, half))
        tgt_other = lax.dynamic_slice(tgt_half, (0, half * (1 - core)), (rows, half))
        mass_all = lax.all_gather(mass_src, 'rows', tiled=True)
        mass_cols = lax.dynamic_slice(mass_tgt, (rows * me,), (rows,))

        gain = (2.0 * ALPHA) * dot('jd,id->ji', feats[:, depth:], feat_all[:, :depth])
        for (lo, hi), (same, cross) in zip(spans, plan_wires):
            near = ordered(start_mine[:, lo:hi], start_pair[:, lo:hi])
            far = ordered(wire.get(same), wire.get(cross))
            prod_a = dot('kj,ki->ji', jnp.concatenate([near, far], axis=0), src_all).astype(jnp.bfloat16)
            both_a = jnp.concatenate([prod_a, swap(prod_a, 1)], axis=0)
            both_c = jnp.concatenate([tgt_mine[:, lo:hi], tgt_other[:, lo:hi]], axis=1)
            gain = gain + (2.0 * (1.0 - ALPHA)) * dot('rj,ji->ri', both_c, both_a)
        plan_t = sinkhorn(group, [gain], mass_cols, mass_all, epsilon, jnp.bfloat16, True, 0)

        tgt_all = assemble(tgt_half, wire.get(tgt_wire))
        part = rows // ROW_PARTS
        src_parts = src_all.reshape(4, ROW_PARTS, part, cols)
        arrived = []
        for h in range(ROW_PARTS):
            blocks = [dot('ik,jk->ij', src_parts[2 + k, h], plan_t).astype(jnp.bfloat16) for k in range(2)]
            arrived.append((wire.send(jnp.where(even, blocks[0], blocks[1]), 2),
                            wire.send(jnp.where(even, blocks[1], blocks[0]), 3)))
        near_blocks = [dot('ik,jk->ij', src_all[k * rows:(k + 1) * rows], plan_t).astype(jnp.bfloat16) for k in range(2)]
        near_mine = jnp.where(even, near_blocks[0], near_blocks[1])
        near_pair = swap(jnp.where(even, near_blocks[1], near_blocks[0]), 1)
        near = ordered(near_mine, near_pair, 1)
        gains = []
        for h in range(ROW_PARTS):
            span = slice(h * part, (h + 1) * part)
            far = ordered(wire.get(arrived[h][0]), wire.get(arrived[h][1]), 1)
            prod_b = dot('ij,jl->il', jnp.concatenate([near[span], far], axis=1), tgt_all)
            cross = dot('id,jd->ij', feats[span, :depth], feat_all[:, depth:])
            gains.append((2.0 * ALPHA) * cross + (2.0 * (1.0 - ALPHA)) * prod_b)
        return sinkhorn(group, gains, mass_src, mass_tgt, epsilon, jnp.float32, False, 1)

    row_spec = P(('pairs', 'rows'), None)
    vec_spec = P(('pairs', 'rows'))
    in_specs = (row_spec, row_spec, row_spec, vec_spec, P('pairs'), row_spec, row_spec, P())
    return jax.shard_map(local_fgw, mesh=mesh, in_specs=in_specs, out_specs=row_spec, check_vma=False)
```

```python
import functools

import jax
import jax.numpy as jnp
from jax import lax
from jax.experimental import pallas as pl
from jax.experimental.pallas import tpu as pltpu
from jax.sharding import PartitionSpec as P

ALPHA = 0.5
SWEEPS = 10
LANES = 128
CHUNKS = 4
BLOCK = 64
LOAD_ROWS = 128
MESH = pl.DeviceIdType.MESH


def sinkhorn_kernel(group, n_gain, transposed, *refs):
    gains, refs = refs[:n_gain], refs[n_gain:]
    (mass_row, mass_col, epsilon, plan_hbm, kern, plan, row_scale, acc, col_scale, shift_fix,
     part_sum, peer_sum, part_top, peer_top, load_sem, store_sem, send_sem, recv_sem, top_send, top_recv) = refs
    rows, cols = kern.shape
    tiles = cols // LANES // CHUNKS
    width = cols // CHUNKS
    gain_rows = rows // n_gain
    me = lax.axis_index('rows')
    chip, core = me // 2, me % 2
    peers = [chip * 2 + (1 - core), (1 - chip) * 2 + core, (1 - chip) * 2 + (1 - core)]

    if transposed:
        loads = [pltpu.make_async_copy(gains[0].at[:, pl.ds(j * width, width)], kern.at[:, pl.ds(j * width, width)],
                                       load_sem.at[j]) for j in range(CHUNKS)]
    else:
        loads = []
        for b in range(rows // LOAD_ROWS):
            start = b * LOAD_ROWS
            source = gains[start // gain_rows].at[pl.ds(start % gain_rows, LOAD_ROWS)]
            loads.append(pltpu.make_async_copy(source, kern.at[pl.ds(start, LOAD_ROWS)], load_sem.at[b]))
    for load in loads:
        load.start()

    barrier = pltpu.get_barrier_semaphore()
    for peer in peers:
        pl.semaphore_signal(barrier, inc=1, device_id={'rows': peer}, device_id_type=MESH)
    pl.semaphore_wait(barrier, group - 1)

    def tile(j, t):
        start = j * width + t * LANES
        return slice(start, start + LANES)

    def sends(slot, j):
        return [pltpu.make_async_remote_copy(
            src_ref=part_sum.at[slot, j], dst_ref=peer_sum.at[slot, k, j], send_sem=send_sem.at[slot, k, j],
            recv_sem=recv_sem.at[slot, k, j], device_id={'rows': peers[k]}, device_id_type=MESH) for k in range(group - 1)]

    def top_sends(j):
        return [pltpu.make_async_remote_copy(
            src_ref=part_top.at[j], dst_ref=peer_top.at[k, j], send_sem=top_send.at[k, j],
            recv_sem=top_recv.at[k, j], device_id={'rows': peers[k]}, device_id_type=MESH) for k in range(group - 1)]

    inv_eps = 1.0 / epsilon[0]

    def split(val):
        return val.reshape(val.shape[0] // 8, 8, LANES)

    def row_update():
        for h in range(0, rows, 256):
            span = slice(h, h + 256)
            row_scale[span, :] = mass_row[span, :] / jnp.sum(acc[span, :], axis=1, keepdims=True)

    def col_pass(slot, j):
        def body(i, sums):
            span = pl.ds(i * BLOCK, BLOCK)
            scale = split(row_scale[span, :])
            return tuple(sums[t] + jnp.sum(split(kern[span, tile(j, t)]) * scale, axis=0) for t in range(tiles))
        sums = lax.fori_loop(0, rows // BLOCK, body, tuple(jnp.zeros((8, LANES), jnp.float32) for _ in range(tiles)))
        total = jnp.concatenate([jnp.sum(s, axis=0, keepdims=True) for s in sums], axis=0)
        if transposed:
            total = total * shift_fix[j]
        part_sum[slot, j] = total
        for send in sends(slot, j):
            send.start()

    def col_update(slot, j):
        for send in sends(slot, j):
            send.wait()
        total = part_sum[slot, j]
        for k in range(group - 1):
            total = total + peer_sum[slot, k, j]
        scale = mass_col[j] / total
        if transposed:
            scale = scale * shift_fix[j]
        col_scale[j] = scale

    def scale_rows(j):
        return [jnp.broadcast_to(col_scale[j, t:t + 1, :], (8, LANES)) for t in range(tiles)]

    def row_pass(j):
        scale = scale_rows(j)

        def body(i, carry):
            span = pl.ds(i * BLOCK, BLOCK)
            total = None if j == 0 else split(acc[span, :])
            for t in range(tiles):
                term = split(kern[span, tile(j, t)]) * scale[t][None]
                total = term if total is None else total + term
            acc[span, :] = total.reshape(BLOCK, LANES)
            return carry
        lax.fori_loop(0, rows // BLOCK, body, 0)

    def plan_chunk(j):
        scale = scale_rows(j)

        def plan_block(i, carry):
            span = pl.ds(i * BLOCK, BLOCK)
            left = split(row_scale[span, :])
            for t in range(tiles):
                val = left * split(kern[span, tile(j, t)]) * scale[t][None]
                plan[span, tile(j, t)] = val.reshape(BLOCK, LANES).astype(plan.dtype)
            return carry
        lax.fori_loop(0, rows // BLOCK, plan_block, 0)
        span = pl.ds(j * width, width)
        store = pltpu.make_async_copy(plan.at[:, span], plan_hbm.at[:, span], store_sem.at[j])
        store.start()
        return store

    if transposed:
        for j in range(CHUNKS):
            loads[j].wait()

            def top_block(i, tops, j=j):
                span = pl.ds(i * BLOCK, BLOCK)
                return tuple(jnp.maximum(tops[t], jnp.max(split(kern[span, tile(j, t)]), axis=0)) for t in range(tiles))
            tops = lax.fori_loop(0, rows // BLOCK, top_block,
                                 tuple(kern[0:8, tile(j, t)] for t in range(tiles)))
            tops = [jnp.max(top, axis=0, keepdims=True) for top in tops]
            wide = [jnp.broadcast_to(top, (8, LANES)) for top in tops]

            def exp_block(i, sums, j=j, wide=wide):
                span = pl.ds(i * BLOCK, BLOCK)
                out = []
                for t in range(tiles):
                    val = jnp.exp((split(kern[span, tile(j, t)]) - wide[t][None]) * inv_eps)
                    kern[span, tile(j, t)] = val.reshape(BLOCK, LANES)
                    out.append(sums[t] + jnp.sum(val, axis=0))
                return tuple(out)
            sums = lax.fori_loop(0, rows // BLOCK, exp_block,
                                 tuple(jnp.zeros((8, LANES), jnp.float32) for _ in range(tiles)))
            part_top[j, 0] = jnp.concatenate(tops, axis=0)
            part_top[j, 1] = jnp.concatenate([jnp.sum(s, axis=0, keepdims=True) for s in sums], axis=0)
            for send in top_sends(j):
                send.start()
        for j in range(CHUNKS):
            for send in top_sends(j):
                send.wait()
            top = part_top[j, 0]
            for k in range(group - 1):
                top = jnp.maximum(top, peer_top[k, j, 0])
            fix = jnp.exp((part_top[j, 0] - top) * inv_eps)
            total = part_top[j, 1] * fix
            for k in range(group - 1):
                total = total + peer_top[k, j, 1] * jnp.exp((peer_top[k, j, 0] - top) * inv_eps)
            shift_fix[j] = fix
            col_scale[j] = mass_col[j] / total * fix
            row_pass(j)
        row_update()
    else:
        for b, load in enumerate(loads):
            load.wait()

            def exp_rows(i, carry, b=b):
                span = pl.ds(b * LOAD_ROWS + i * BLOCK, BLOCK)
                top = kern[span, 0:LANES]
                for t in range(1, cols // LANES):
                    top = jnp.maximum(top, kern[span, t * LANES:(t + 1) * LANES])
                top = jnp.max(top, axis=1, keepdims=True)
                total = jnp.zeros((BLOCK, LANES), jnp.float32)
                for t in range(cols // LANES):
                    val = jnp.exp((kern[span, t * LANES:(t + 1) * LANES] - top) * inv_eps)
                    kern[span, t * LANES:(t + 1) * LANES] = val
                    total = total + val
                acc[span, :] = total
                return carry
            lax.fori_loop(0, LOAD_ROWS // BLOCK, exp_rows, 0)
        row_update()

    def sweep(n, carry):
        slot = lax.rem(n, 2)
        for j in range(CHUNKS):
            col_pass(slot, j)
        for j in range(CHUNKS):
            col_update(slot, j)
            row_pass(j)
        row_update()
        return carry
    lax.fori_loop(0, SWEEPS - 1, sweep, 0)

    stores = []
    if transposed:
        for j in range(CHUNKS):
            stores.append(plan_chunk(j))
    else:
        last = (SWEEPS - 1) % 2
        for j in range(CHUNKS):
            col_pass(last, j)
        for j in range(CHUNKS):
            col_update(last, j)
            stores.append(plan_chunk(j))
    for store in stores:
        store.wait()


def sinkhorn(group, gains, mass_row, mass_col, epsilon, dtype, transposed, collective_id):
    cols = gains[0].shape[1]
    rows = sum(g.shape[0] for g in gains)
    tiles = cols // LANES // CHUNKS
    row_rep = jnp.broadcast_to(mass_row[:, None], (rows, LANES))
    col_tiles = mass_col.reshape(CHUNKS, tiles, LANES)
    n_load = CHUNKS if transposed else rows // LOAD_ROWS
    vec = (CHUNKS, tiles, LANES)
    pair = (CHUNKS, 2, tiles, LANES)
    return pl.pallas_call(
        functools.partial(sinkhorn_kernel, group, len(gains), transposed),
        out_shape=jax.ShapeDtypeStruct((rows, cols), dtype),
        in_specs=[pl.BlockSpec(memory_space=pl.ANY)] * len(gains) + [
            pl.BlockSpec(memory_space=pltpu.VMEM), pl.BlockSpec(memory_space=pltpu.VMEM),
            pl.BlockSpec(memory_space=pltpu.SMEM)],
        out_specs=pl.BlockSpec(memory_space=pl.ANY),
        scratch_shapes=[
            pltpu.VMEM((rows, cols), jnp.float32),
            pltpu.VMEM((rows, cols), dtype),
            pltpu.VMEM((rows, LANES), jnp.float32),
            pltpu.VMEM((rows, LANES), jnp.float32),
            pltpu.VMEM(vec, jnp.float32),
            pltpu.VMEM(vec, jnp.float32),
            pltpu.VMEM((2,) + vec, jnp.float32),
            pltpu.VMEM((2, group - 1) + vec, jnp.float32),
            pltpu.VMEM(pair, jnp.float32),
            pltpu.VMEM((group - 1,) + pair, jnp.float32),
            pltpu.SemaphoreType.DMA((n_load,)),
            pltpu.SemaphoreType.DMA((CHUNKS,)),
            pltpu.SemaphoreType.DMA((2, group - 1, CHUNKS)),
            pltpu.SemaphoreType.DMA((2, group - 1, CHUNKS)),
            pltpu.SemaphoreType.DMA((group - 1, CHUNKS)),
            pltpu.SemaphoreType.DMA((group - 1, CHUNKS)),
        ],
        compiler_params=pltpu.CompilerParams(collective_id=collective_id, has_side_effects=True,
                                             vmem_limit_bytes=48 * 1024 * 1024),
        cost_estimate=pl.CostEstimate(flops=4 * SWEEPS * rows * cols, bytes_accessed=8 * rows * cols,
                                      transcendentals=rows * cols),
        name='sinkhorn_cols' if transposed else 'sinkhorn_rows',
    )(*gains, row_rep, col_tiles, epsilon.reshape(1))


STEP = 256
SLAB = 512
NT = (((1,), (1,)), ((), ()))
NN = (((1,), (0,)), ((), ()))


def weighted(value, factor):
    return value if factor == 1.0 else value * factor


def mm(left, right, dims):
    return lax.dot_general(left, right, dims, preferred_element_type=jnp.float32)


class Links:
    def __init__(self, send_sem, recv_sem):
        self.send_sem, self.recv_sem = send_sem, recv_sem

    def copy(self, source, target, peer, index):
        return pltpu.make_async_remote_copy(src_ref=source, dst_ref=target, send_sem=self.send_sem.at[index],
                                            recv_sem=self.recv_sem.at[index], device_id={'rows': peer}, device_id_type=MESH)


def places():
    me = lax.axis_index('rows')
    chip, core = me // 2, me % 2
    return me, chip, core, chip * 2 + (1 - core), (1 - chip) * 2 + core, (1 - chip) * 2 + (1 - core)


def entry_barrier(peers):
    barrier = pltpu.get_barrier_semaphore()
    for peer in peers:
        pl.semaphore_signal(barrier, inc=1, device_id={'rows': peer}, device_id_type=MESH)
    pl.semaphore_wait(barrier, len(peers))


def block_sources(cost, me, core, rows):
    quad = rows // 2
    diag = me * rows
    off = (me + 1 - 2 * core) * rows

    def at(row, col):
        return cost.at[pl.ds(pl.multiple_of(row, quad), quad), pl.ds(pl.multiple_of(col, quad), quad)]
    return [at(0, diag), at(0, diag + quad), at(quad, diag + quad), at(0, off + quad * core), at(quad * core, off + quad)]


def assemble(cost, cost_near, blocks, far, slab, turned, sems, chip, core, rows):
    quad = rows // 2
    half = 2 * rows
    away = half * (1 - chip)
    for source, owner in ((cost, core), (cost_near, 1 - core)):
        for a in range(rows // SLAB):
            load = pltpu.make_async_copy(source.at[pl.ds(a * SLAB, SLAB), pl.ds(pl.multiple_of(away, half), half)], slab, sems.at[0])
            load.start()
            load.wait()

            def turn(b, carry):
                turned[pl.ds(pl.multiple_of(b * SLAB, SLAB), SLAB), :] = slab[:, pl.ds(pl.multiple_of(b * SLAB, SLAB), SLAB)].T
                return carry
            lax.fori_loop(0, half // SLAB, turn, 0)
            col = pl.multiple_of(half * chip + owner * rows + a * SLAB, SLAB)
            store = pltpu.make_async_copy(turned, far.at[:, pl.ds(col, SLAB)], sems.at[1])
            store.start()
            store.wait()

    def corner(k, carry):
        cc = core + k - 2 * core * k
        base, other = cc * rows, (1 - cc) * rows
        spots = [(base, base), (base, base + quad), (base + quad, base + quad),
                 (base, other + quad * cc), (base + quad * cc, other + quad)]
        loads = [pltpu.make_async_copy(blocks.at[k, b], slab.at[:, pl.ds(b % 4 * quad, quad)] if b < 4 else
                                       turned.at[pl.ds(3 * quad, quad), :], sems.at[2 + b]) for b in range(5)]
        for load in loads:
            load.start()
        for load in loads:
            load.wait()
        turned[pl.ds(0, quad), :] = slab[:, quad:2 * quad].T
        turned[pl.ds(quad, quad), :] = slab[:, 3 * quad:4 * quad].T
        turned[pl.ds(2 * quad, quad), :] = turned[pl.ds(3 * quad, quad), :].T
        stores = []

        def put(source, row, col):
            target = far.at[pl.ds(pl.multiple_of(row, quad), quad), pl.ds(pl.multiple_of(away + col, quad), quad)]
            stores.append(pltpu.make_async_copy(source, target, sems.at[7 + len(stores)]))
            stores[-1].start()
        for b in range(4):
            put(slab.at[:, pl.ds(b * quad, quad)], *spots[b])
        put(turned.at[pl.ds(3 * quad, quad), :], *spots[4])
        for t, b in enumerate((1, 3, 4)):
            put(turned.at[pl.ds(t * quad, quad), :], spots[b][1], spots[b][0])
        for store in stores:
            store.wait()
        return carry
    lax.fori_loop(0, 2, corner, 0)


def first_kernel(src, tgt, start, feats, gain, src_near, src_blocks, src_far, tgt_near, tgt_blocks, feat_peer,
                 start_near, start_far, acc, tgt_keep, src_buf, start_buf, own_buf, near_buf, slab, turned, feat_buf,
                 load_sem, src_sem, block_sem, send_sem, recv_sem, free_sem):
    rows, cols = src.shape
    half = cols // 2
    steps = half // STEP
    me, chip, core, near, same, cross = places()
    links = Links(send_sem, recv_sem)
    keep = pltpu.make_async_copy(tgt, tgt_keep, load_sem.at[0])
    keep.start()
    entry_barrier((near, same, cross))

    def col_span(base, s):
        return pl.ds(pl.multiple_of(base + s * STEP, STEP), STEP)

    mine, other = half * core, half * (1 - core)
    local = [links.copy(src, src_near, near, 0),
             links.copy(feats, feat_peer.at[0], near, 1),
             links.copy(start.at[:, pl.ds(pl.multiple_of(other, half), half)], start_near, near, 2),
             links.copy(tgt, tgt_near, near, 3)]
    src_out = [links.copy(block, src_blocks.at[0, b], same, 4 + b) for b, block in enumerate(block_sources(src, me, core, rows))]
    feat_out = links.copy(feats, feat_peer.at[1], same, 9)
    tgt_out = [links.copy(block, tgt_blocks.at[0, b], same, 10 + b) for b, block in enumerate(block_sources(tgt, me, core, rows))]
    src_pass = links.copy(src_blocks.at[0], src_blocks.at[1], near, 15)
    feat_pass = links.copy(feat_peer.at[1], feat_peer.at[2], near, 16)
    tgt_pass = links.copy(tgt_blocks.at[0], tgt_blocks.at[1], near, 17)

    def start_out(s):
        return [links.copy(start.at[:, col_span(mine, s)], start_far.at[0, :, col_span(0, s)], same, 18 + s),
                links.copy(start.at[:, col_span(other, s)], start_far.at[1, :, col_span(0, s)], cross, 18 + steps + s)]

    def near_copy(s, slot):
        return links.copy(own_buf.at[slot], near_buf.at[slot], near, 18 + 2 * steps + slot)

    for copy in local[:3] + src_out + [feat_out]:
        copy.start()
    for s in range(steps):
        for copy in start_out(s):
            copy.start()
    for copy in tgt_out + [local[3]]:
        copy.start()

    for copy in src_out:
        copy.wait_recv()
    src_pass.start()
    local[0].wait_recv()
    src_pass.wait_recv()
    assemble(src, src_near, src_blocks, src_far, slab, turned, block_sem, chip, core, rows)

    feat_out.wait_recv()
    feat_pass.start()
    local[1].wait_recv()
    feat_pass.wait_recv()
    depth = feats.shape[1] // 2
    own_feat = pltpu.make_async_copy(feats, feat_buf.at[0], load_sem.at[1])
    own_feat.start()
    own_feat.wait()
    for k, device in enumerate((me, near, same, cross)):
        source = feats if k == 0 else feat_peer.at[k - 1]
        load = pltpu.make_async_copy(source, feat_buf.at[1], load_sem.at[1])
        load.start()
        load.wait()

        def cross_term(h, carry, device=device):
            block = mm(feat_buf[0, :, depth:], feat_buf[1, pl.ds(pl.multiple_of(h * 256, 256), 256), :depth], NT)
            acc[:, pl.ds(pl.multiple_of(device * rows + h * 256, 256), 256)] = weighted(block, 2.0 * ALPHA)
            return carry
        lax.fori_loop(0, rows // 256, cross_term, 0)
    keep.wait()

    per = rows // SLAB
    n_blocks = 4 * per

    def src_load(b):
        if b < per:
            source = src.at[pl.ds(b * SLAB, SLAB)]
        elif b < 2 * per:
            source = src_near.at[pl.ds((b - per) * SLAB, SLAB)]
        else:
            source = src_far.at[pl.ds((b - 2 * per) * SLAB, SLAB)]
        return pltpu.make_async_copy(source, src_buf.at[b % 2], src_sem.at[b % 2])

    def row_of(b):
        if b < per:
            return me * rows + b * SLAB
        if b < 2 * per:
            return near * rows + (b - per) * SLAB
        return (1 - chip) * half + (b - 2 * per) * SLAB

    def gather(left_base, left_s, right, slot):
        def update(h, carry):
            span = pl.ds(pl.multiple_of(h * 512, 512), 512)
            block = mm(tgt_keep[:, col_span(left_base, left_s)], right[slot, span, :], NT)
            acc[:, span] += weighted(block, 2.0 * (1.0 - ALPHA))
            return carry
        lax.fori_loop(0, cols // 512, update, 0)

    local[2].wait_recv()
    src_load(0).start()

    def step(s, carry):
        slot = lax.rem(s, 2)
        for copy in start_out(s):
            copy.wait_recv()
        loads = []
        for k, device in enumerate((me, near, same, cross)):
            source = (start.at[:, col_span(mine, s)] if k == 0 else start_near.at[:, col_span(0, s)] if k == 1
                      else start_far.at[k - 2, :, col_span(0, s)])
            loads.append(pltpu.make_async_copy(source, start_buf.at[pl.ds(pl.multiple_of(device * rows, rows), rows)],
                                               load_sem.at[2 + k]))
        for load in loads:
            load.start()

        @pl.when(s >= 2)
        def _():
            near_copy(s - 2, slot).wait_send()
        for load in loads:
            load.wait()
        for b in range(n_blocks):
            src_load(b).wait()
            if b + 1 < n_blocks:
                src_load(b + 1).start()
            else:
                @pl.when(s + 1 < steps)
                def _():
                    src_load(0).start()
            own_buf[slot, pl.ds(pl.multiple_of(row_of(b), SLAB), SLAB), :] = mm(src_buf[b % 2], start_buf[...], NN).astype(jnp.bfloat16)

        @pl.when(s >= 2)
        def _():
            pl.semaphore_wait(free_sem, 1)
        near_copy(s, slot).start()
        gather(mine, s, own_buf, slot)

        @pl.when(s >= 1)
        def _():
            near_copy(s - 1, 1 - slot).wait_recv()
            gather(other, s - 1, near_buf, 1 - slot)

        @pl.when(jnp.logical_and(s >= 1, s - 1 < steps - 2))
        def _():
            pl.semaphore_signal(free_sem, inc=1, device_id={'rows': near}, device_id_type=MESH)
        return carry
    lax.fori_loop(0, steps, step, 0)
    final = (steps - 1) % 2
    near_copy(steps - 1, final).wait_recv()
    gather(other, steps - 1, near_buf, final)
    store = pltpu.make_async_copy(acc, gain, load_sem.at[0])
    store.start()
    for copy in tgt_out:
        copy.wait_recv()
    tgt_pass.start()
    local[3].wait_recv()
    tgt_pass.wait_recv()
    for slot in range(2):
        near_copy(0, slot).wait_send()
    for copy in local + src_out + [feat_out] + tgt_out + [src_pass, feat_pass, tgt_pass]:
        copy.wait_send()
    for s in range(steps):
        for copy in start_out(s):
            copy.wait_send()
    store.wait()


def first_step(src, tgt, start, feats):
    rows, cols = src.shape
    quad = rows // 2
    half = cols // 2
    steps = half // STEP
    n_links = 18 + 2 * steps + 2
    any_spec = pl.BlockSpec(memory_space=pl.ANY)
    bf16 = jnp.bfloat16
    shapes = [((rows, cols), jnp.float32), ((rows, cols), bf16), ((2, 5, quad, quad), bf16), ((half, cols), bf16),
              ((rows, cols), bf16), ((2, 5, quad, quad), bf16), ((3,) + feats.shape, bf16),
              ((rows, half), bf16), ((2, rows, half), bf16)]
    return pl.pallas_call(
        first_kernel,
        out_shape=[jax.ShapeDtypeStruct(*s) for s in shapes],
        in_specs=[any_spec] * 4,
        out_specs=[any_spec] * len(shapes),
        scratch_shapes=[
            pltpu.VMEM((rows, cols), jnp.float32),
            pltpu.VMEM((rows, cols), bf16),
            pltpu.VMEM((2, SLAB, cols), bf16),
            pltpu.VMEM((cols, STEP), bf16),
            pltpu.VMEM((2, cols, STEP), bf16),
            pltpu.VMEM((2, cols, STEP), bf16),
            pltpu.VMEM((SLAB, half), bf16),
            pltpu.VMEM((half, SLAB), bf16),
            pltpu.VMEM((2,) + feats.shape, bf16),
            pltpu.SemaphoreType.DMA((6,)),
            pltpu.SemaphoreType.DMA((2,)),
            pltpu.SemaphoreType.DMA((15,)),
            pltpu.SemaphoreType.DMA((n_links,)),
            pltpu.SemaphoreType.DMA((n_links,)),
            pltpu.SemaphoreType.REGULAR,
        ],
        compiler_params=pltpu.CompilerParams(collective_id=2, has_side_effects=True, vmem_limit_bytes=62 * 1024 * 1024),
        cost_estimate=pl.CostEstimate(flops=6 * rows * cols * cols, bytes_accessed=400000000, transcendentals=0),
        name='first_step',
    )(src, tgt, start, feats)


def second_kernel(plan_t, src, src_near, src_far, tgt, tgt_near, tgt_blocks, feats, feat_peer, gain, tgt_far,
                  acc, plan_keep, src_buf, made, ready, slab, turned, feat_buf,
                  load_sem, src_sem, block_sem, send_sem, recv_sem):
    rows, cols = src.shape
    half = cols // 2
    me, chip, core, near, same, cross = places()
    links = Links(send_sem, recv_sem)
    per = rows // SLAB
    keep = pltpu.make_async_copy(plan_t, plan_keep, load_sem.at[0])
    keep.start()
    entry_barrier((near, same, cross))

    def block(matrix, matrix_near, matrix_far, k, h):
        if k == 0:
            return matrix.at[pl.ds(h * SLAB, SLAB)]
        if k == 1:
            return matrix_near.at[pl.ds(h * SLAB, SLAB)]
        which = core if k == 2 else 1 - core
        return matrix_far.at[pl.ds(pl.multiple_of(which * rows + h * SLAB, SLAB), SLAB)]

    order = [(k, h) for k in (2, 3, 1, 0) for h in range(per)]
    devices = (me, near, same, cross)

    def src_load(n):
        k, h = order[n]
        return pltpu.make_async_copy(block(src, src_near, src_far, k, h), src_buf.at[n % 2], src_sem.at[n % 2])

    column = pl.ds(pl.multiple_of(me * rows, rows), rows)
    copies = []
    src_load(0).start()
    keep.wait()
    for n, (k, h) in enumerate(order):
        src_load(n).wait()
        if n + 1 < len(order):
            src_load(n + 1).start()

        def make(t, carry, n=n, k=k, h=h):
            span = pl.ds(pl.multiple_of(t * 256, 256), 256)
            value = mm(src_buf[n % 2], plan_keep[span, :], NT).astype(jnp.bfloat16)
            if k == 0:
                ready[pl.ds(h * SLAB, SLAB), pl.ds(pl.multiple_of(me * rows + t * 256, 256), 256)] = value
            else:
                made[n, :, span] = value
            return carry
        lax.fori_loop(0, rows // 256, make, 0)
        if k:
            copies.append(links.copy(made.at[n], ready.at[pl.ds(h * SLAB, SLAB), column], devices[k], n))
            copies[-1].start()

    def tgt_load(n):
        k, h = turn[n]
        return pltpu.make_async_copy(block(tgt, tgt_near, tgt_far, k, h), src_buf.at[n % 2], src_sem.at[n % 2])

    depth = feats.shape[1] // 2
    own_feat = pltpu.make_async_copy(feats, feat_buf.at[0], load_sem.at[1])
    own_feat.start()
    own_feat.wait()
    for k, device in enumerate(devices):
        source = feats if k == 0 else feat_peer.at[k - 1]
        load = pltpu.make_async_copy(source, feat_buf.at[1], load_sem.at[1])
        load.start()
        load.wait()

        def cross_term(h, carry, device=device):
            value = mm(feat_buf[0, :, :depth], feat_buf[1, pl.ds(pl.multiple_of(h * 256, 256), 256), depth:], NT)
            acc[:, pl.ds(pl.multiple_of(device * rows + h * 256, 256), 256)] = weighted(value, 2.0 * ALPHA)
            return carry
        lax.fori_loop(0, rows // 256, cross_term, 0)

    assemble(tgt, tgt_near, tgt_blocks, tgt_far, slab, turned, block_sem, chip, core, rows)
    turn = [(k, h) for k in (0, 1, 2, 3) for h in range(per)]
    tgt_load(0).start()
    for n, (k, h) in enumerate(turn):
        tgt_load(n).wait()
        if n + 1 < len(turn):
            tgt_load(n + 1).start()
        if k and h == 0:
            for copy, (kk, hh) in zip(copies, order):
                if kk == k:
                    copy.wait_recv()
        left = pl.ds(pl.multiple_of(devices[k] * rows + h * SLAB, SLAB), SLAB)

        def update(t, carry, n=n, left=left):
            span = pl.ds(pl.multiple_of(t * 256, 256), 256)
            acc[:, span] += weighted(mm(ready[:, left], src_buf[n % 2, :, span], NN), 2.0 * (1.0 - ALPHA))
            return carry
        lax.fori_loop(0, cols // 256, update, 0)
    store = pltpu.make_async_copy(acc, gain, load_sem.at[0])
    store.start()
    for copy in copies:
        copy.wait_send()
    store.wait()


def second_step(plan_t, src, src_near, src_far, tgt, tgt_near, tgt_blocks, feats, feat_peer):
    rows, cols = src.shape
    half = cols // 2
    n_copies = 3 * rows // SLAB
    any_spec = pl.BlockSpec(memory_space=pl.ANY)
    bf16 = jnp.bfloat16
    gain, _ = pl.pallas_call(
        second_kernel,
        out_shape=[jax.ShapeDtypeStruct((rows, cols), jnp.float32), jax.ShapeDtypeStruct((half, cols), bf16)],
        in_specs=[any_spec] * 9,
        out_specs=[any_spec] * 2,
        scratch_shapes=[
            pltpu.VMEM((rows, cols), jnp.float32),
            pltpu.VMEM((rows, cols), bf16),
            pltpu.VMEM((2, SLAB, cols), bf16),
            pltpu.VMEM((n_copies, SLAB, rows), bf16),
            pltpu.VMEM((rows, cols), bf16),
            pltpu.VMEM((SLAB, half), bf16),
            pltpu.VMEM((half, SLAB), bf16),
            pltpu.VMEM((2,) + feats.shape, bf16),
            pltpu.SemaphoreType.DMA((2,)),
            pltpu.SemaphoreType.DMA((2,)),
            pltpu.SemaphoreType.DMA((15,)),
            pltpu.SemaphoreType.DMA((n_copies,)),
            pltpu.SemaphoreType.DMA((n_copies,)),
        ],
        compiler_params=pltpu.CompilerParams(collective_id=3, has_side_effects=True, vmem_limit_bytes=62 * 1024 * 1024),
        cost_estimate=pl.CostEstimate(flops=4 * rows * cols * cols, bytes_accessed=200000000, transcendentals=0),
        name='second_step',
    )(plan_t, src, src_near, src_far, tgt, tgt_near, tgt_blocks, feats, feat_peer)
    return gain


def solution(mesh):
    group = mesh.shape['rows']

    def local_fgw(cost_src, cost_tgt, plan_init, mass_src, mass_tgt, feat_src, feat_tgt, epsilon):
        rows = cost_src.shape[0]
        me = lax.axis_index('rows')
        src_half = cost_src.astype(jnp.bfloat16)
        tgt_half = cost_tgt.astype(jnp.bfloat16)
        start = plan_init.astype(jnp.bfloat16)
        feats = jnp.concatenate([feat_src, feat_tgt], axis=1).astype(jnp.bfloat16)
        mass_all = lax.all_gather(mass_src, 'rows', tiled=True)
        mass_cols = lax.dynamic_slice(mass_tgt, (rows * me,), (rows,))
        gain, src_near, _, src_far, tgt_near, tgt_blocks, feat_peer, _, _ = first_step(src_half, tgt_half, start, feats)
        plan_t = sinkhorn(group, [gain], mass_cols, mass_all, epsilon, jnp.bfloat16, True, 0)
        gain = second_step(plan_t, src_half, src_near, src_far, tgt_half, tgt_near, tgt_blocks, feats, feat_peer)
        return sinkhorn(group, [gain], mass_src, mass_tgt, epsilon, jnp.float32, False, 1)

    row_spec = P(('pairs', 'rows'), None)
    vec_spec = P(('pairs', 'rows'))
    in_specs = (row_spec, row_spec, row_spec, vec_spec, P('pairs'), row_spec, row_spec, P())
    return jax.shard_map(local_fgw, mesh=mesh, in_specs=in_specs, out_specs=row_spec, check_vma=False)
```

```python
import functools

import jax
import jax.numpy as jnp
from jax import lax
from jax.experimental import pallas as pl
from jax.experimental.pallas import tpu as pltpu
from jax.sharding import PartitionSpec as P

ALPHA = 0.5
SWEEPS = 10
LANES = 128
CHUNKS = 4
BLOCK = 64
STEP = 256
SLAB = 512
TILE = 512
EARLY_STEPS = 1
TAIL_PIECES = 4
GROUP = 4
MESH = pl.DeviceIdType.MESH
NT = (((1,), (1,)), ((), ()))
NN = (((1,), (0,)), ((), ()))
BF16 = jnp.bfloat16
F32 = jnp.float32


def weighted(value, factor):
    return value if factor == 1.0 else value * factor


def mm(left, right, dims):
    return lax.dot_general(left, right, dims, preferred_element_type=F32)


def split(val):
    return val.reshape(val.shape[0] // 8, 8, LANES)


def aligned(start, size):
    return pl.ds(pl.multiple_of(start, size), size)


def assemble(cost, cost_near, blocks, far, slab, turned, sems, chip, core, rows):
    quad = rows // 2
    half = 2 * rows
    away = half * (1 - chip)
    for source, owner in ((cost, core), (cost_near, 1 - core)):
        for a in range(rows // SLAB):
            load = pltpu.make_async_copy(source.at[pl.ds(a * SLAB, SLAB), aligned(away, half)], slab, sems.at[0])
            load.start()
            load.wait()

            def turn(b, carry):
                turned[aligned(b * SLAB, SLAB), :] = slab[:, aligned(b * SLAB, SLAB)].T
                return carry
            lax.fori_loop(0, half // SLAB, turn, 0)
            store = pltpu.make_async_copy(turned, far.at[:, aligned(half * chip + owner * rows + a * SLAB, SLAB)], sems.at[1])
            store.start()
            store.wait()

    def corner(k, carry):
        cc = core + k - 2 * core * k
        base, other = cc * rows, (1 - cc) * rows
        spots = [(base, base), (base, base + quad), (base + quad, base + quad),
                 (base, other + quad * cc), (base + quad * cc, other + quad)]
        loads = [pltpu.make_async_copy(blocks.at[k, b], slab.at[:, pl.ds(b * quad, quad)] if b < 4 else
                                       turned.at[pl.ds(3 * quad, quad), :], sems.at[2 + b]) for b in range(5)]
        for load in loads:
            load.start()
        for load in loads:
            load.wait()
        turned[pl.ds(0, quad), :] = slab[:, quad:2 * quad].T
        turned[pl.ds(quad, quad), :] = slab[:, 3 * quad:4 * quad].T
        turned[pl.ds(2 * quad, quad), :] = turned[pl.ds(3 * quad, quad), :].T
        stores = []

        def put(source, row, col):
            target = far.at[aligned(row, quad), aligned(away + col, quad)]
            stores.append(pltpu.make_async_copy(source, target, sems.at[7 + len(stores)]))
            stores[-1].start()
        for b in range(4):
            put(slab.at[:, pl.ds(b * quad, quad)], *spots[b])
        put(turned.at[pl.ds(3 * quad, quad), :], *spots[4])
        for t, b in enumerate((1, 3, 4)):
            put(turned.at[pl.ds(t * quad, quad), :], spots[b][1], spots[b][0])
        for store in stores:
            store.wait()
        return carry
    lax.fori_loop(0, 2, corner, 0)


def kernel(src_f32, tgt_f32, start, feat_src, feat_tgt, mass_mine, mass_rows_t, mass_rows, mass_cols, epsilon,
           kern_out, row_out, col_out, src, tgt, src_near, src_blocks, src_far, tgt_near, tgt_blocks, tgt_far,
           src_feat_peer, tgt_feat_peer, start_near, start_far, ready,
           acc, keep, src_buf, start_buf, own_buf, near_buf, made, left_buf, slab, turned, feat_buf, mass_all,
           row_scale, row_acc, col_scale, shift_fix, part_sum, peer_sum, part_top, peer_top,
           load_sem, src_sem, block_sem, send_sem, recv_sem, sum_send, sum_recv, top_send, top_recv, free_sem):
    rows, cols = src_f32.shape
    half = cols // 2
    quad = rows // 2
    steps = half // STEP
    per = rows // SLAB
    tiles = cols // LANES // CHUNKS
    width = cols // CHUNKS
    me = lax.axis_index('rows')
    chip, core = me // 2, me % 2
    near, same, cross = chip * 2 + (1 - core), (1 - chip) * 2 + core, (1 - chip) * 2 + (1 - core)
    peers = (near, same, cross)
    devices = (me, near, same, cross)
    inv_eps = 1.0 / epsilon[0]

    src_load_all = [pltpu.make_async_copy(src_f32.at[pl.ds(b * quad, quad)], acc.at[pl.ds(b * quad, quad)], load_sem.at[b])
                    for b in range(2)]
    for load in src_load_all:
        load.start()
    mass_all[me] = mass_mine[...]
    barrier = pltpu.get_barrier_semaphore()
    for peer in peers:
        pl.semaphore_signal(barrier, inc=1, device_id={'rows': peer}, device_id_type=MESH)
    pl.semaphore_wait(barrier, GROUP - 1)

    counter = [0]

    def reserve(count):
        counter[0] += count
        return counter[0] - count

    def remote(source, target, peer, index):
        return pltpu.make_async_remote_copy(src_ref=source, dst_ref=target, send_sem=send_sem.at[index],
                                            recv_sem=recv_sem.at[index], device_id={'rows': peer}, device_id_type=MESH)

    def col_span(base, s):
        return aligned(base + s * STEP, STEP)

    def block_spots():
        diag, off = me * rows, (me + 1 - 2 * core) * rows
        return [(0, diag), (0, diag + quad), (quad, diag + quad), (0, off + quad * core), (quad * core, off + quad)]

    mine, other = half * core, half * (1 - core)
    src_near_out = remote(src, src_near, near, reserve(1))
    src_feat_near = remote(feat_src, src_feat_peer.at[0], near, reserve(1))
    start_near_out = remote(start.at[:, aligned(other, half)], start_near, near, reserve(1))
    tgt_near_out = remote(tgt, tgt_near, near, reserve(1))
    tgt_feat_near = remote(feat_tgt, tgt_feat_peer.at[0], near, reserve(1))
    src_out = [remote(src.at[aligned(row, quad), aligned(col, quad)], src_blocks.at[0, b], same, reserve(1))
               for b, (row, col) in enumerate(block_spots())]
    src_feat_out = remote(feat_src, src_feat_peer.at[1], same, reserve(1))
    tgt_feat_out = remote(feat_tgt, tgt_feat_peer.at[1], same, reserve(1))
    piece = quad // 2
    tgt_out = [remote(tgt.at[aligned(row + h * piece, piece), aligned(col, quad)],
                      tgt_blocks.at[0, b, pl.ds(h * piece, piece)], same, reserve(1))
               for b, (row, col) in enumerate(block_spots()) for h in range(2)]
    src_pass = remote(src_blocks.at[0], src_blocks.at[1], near, reserve(1))
    src_feat_pass = remote(src_feat_peer.at[1], src_feat_peer.at[2], near, reserve(1))
    tgt_pass = remote(tgt_blocks.at[0], tgt_blocks.at[1], near, reserve(1))
    tgt_feat_pass = remote(tgt_feat_peer.at[1], tgt_feat_peer.at[2], near, reserve(1))
    mass_out = [remote(mass_mine, mass_all.at[me], peer, reserve(1)) for peer in peers]
    start_base = reserve(2 * steps)
    near_base = reserve(2)
    late_pieces = tgt_out[TAIL_PIECES:] + [tgt_feat_out]

    def start_out(s):
        return [remote(start.at[:, col_span(mine, s)], start_far.at[0, :, col_span(0, s)], same, start_base + s),
                remote(start.at[:, col_span(other, s)], start_far.at[1, :, col_span(0, s)], cross, start_base + steps + s)]

    def near_copy(slot):
        return remote(own_buf.at[slot], near_buf.at[slot], near, near_base + slot)

    for s in range(EARLY_STEPS):
        for copy in start_out(s):
            copy.start()
    for copy in [start_near_out, src_feat_near, tgt_feat_near] + mass_out:
        copy.start()

    src_stores = []
    for b in range(2):
        src_load_all[b].wait()

        def cast(t, carry, b=b):
            span = aligned(t * BLOCK, BLOCK)
            src_buf[b, span, :] = acc[aligned(b * quad + t * BLOCK, BLOCK), :].astype(BF16)
            return carry
        lax.fori_loop(0, quad // BLOCK, cast, 0)
        src_stores.append(pltpu.make_async_copy(src_buf.at[b], src.at[pl.ds(b * quad, quad)], src_sem.at[b]))
        src_stores[-1].start()
    tgt_load_all = pltpu.make_async_copy(tgt_f32, acc, load_sem.at[0])
    tgt_load_all.start()
    for store in src_stores:
        store.wait()
    for copy in src_out + [src_near_out, src_feat_out]:
        copy.start()
    for s in range(EARLY_STEPS, steps):
        for copy in start_out(s):
            copy.start()
    tgt_load_all.wait()

    def cast_tgt(t, carry):
        span = aligned(t * BLOCK, BLOCK)
        keep[span, :] = acc[span, :].astype(BF16)
        return carry
    lax.fori_loop(0, rows // BLOCK, cast_tgt, 0)
    tgt_store = pltpu.make_async_copy(keep, tgt, load_sem.at[0])
    tgt_store.start()
    tgt_store.wait()
    tgt_near_out.start()
    for copy in tgt_out[:TAIL_PIECES]:
        copy.start()

    def cross_terms(first, peer_second):
        own = pltpu.make_async_copy(first, feat_buf.at[0], load_sem.at[1])
        own.start()
        own.wait()
        for k, device in enumerate(devices):
            load = pltpu.make_async_copy(peer_second(k), feat_buf.at[1], load_sem.at[1])
            load.start()
            load.wait()

            def cross_term(h, carry, device=device):
                block = mm(feat_buf[0], feat_buf[1, aligned(h * 256, 256), :], NT)
                acc[:, aligned(device * rows + h * 256, 256)] = weighted(block, 2.0 * ALPHA)
                return carry
            lax.fori_loop(0, rows // 256, cross_term, 0)

    src_feat_near.wait_recv()
    for copy in src_out:
        copy.wait_recv()
    src_pass.start()
    src_feat_out.wait_recv()
    src_feat_pass.start()
    src_near_out.wait_recv()
    src_pass.wait_recv()
    assemble(src, src_near, src_blocks, src_far, slab, turned, block_sem, chip, core, rows)
    src_feat_pass.wait_recv()
    cross_terms(feat_tgt, lambda k: feat_src if k == 0 else src_feat_peer.at[k - 1])

    def rows_of(matrix, matrix_near, matrix_far, k, h):
        if k == 0:
            return matrix.at[pl.ds(h * SLAB, SLAB)]
        if k == 1:
            return matrix_near.at[pl.ds(h * SLAB, SLAB)]
        which = core if k == 2 else 1 - core
        return matrix_far.at[aligned(which * rows + h * SLAB, SLAB)]

    ordered = [(k, h) for k in range(GROUP) for h in range(per)]

    def src_load(b):
        return pltpu.make_async_copy(rows_of(src, src_near, src_far, *ordered[b]), src_buf.at[b % 2], src_sem.at[b % 2])

    def gather(base, s, right, slot):
        def update(h, carry):
            span = aligned(h * TILE, TILE)
            block = mm(keep[:, col_span(base, s)], right[slot, span, :], NT)
            acc[:, span] += weighted(block, 2.0 * (1.0 - ALPHA))
            return carry
        lax.fori_loop(0, cols // TILE, update, 0)

    start_near_out.wait_recv()
    src_load(0).start()

    def step(s, carry):
        slot = lax.rem(s, 2)
        for copy in start_out(s):
            copy.wait_recv()
        loads = []
        for k, device in enumerate(devices):
            source = (start.at[:, col_span(mine, s)] if k == 0 else start_near.at[:, col_span(0, s)] if k == 1
                      else start_far.at[k - 2, :, col_span(0, s)])
            loads.append(pltpu.make_async_copy(source, start_buf.at[aligned(device * rows, rows)], load_sem.at[2 + k]))
        for load in loads:
            load.start()

        @pl.when(s >= 2)
        def _():
            near_copy(slot).wait_send()
        for load in loads:
            load.wait()
        for b, (k, h) in enumerate(ordered):
            src_load(b).wait()
            if b + 1 < len(ordered):
                src_load(b + 1).start()
            else:
                @pl.when(s + 1 < steps)
                def _():
                    src_load(0).start()
            own_buf[slot, aligned(devices[k] * rows + h * SLAB, SLAB), :] = mm(src_buf[b % 2], start_buf[...], NN).astype(BF16)

        @pl.when(s >= 2)
        def _():
            pl.semaphore_wait(free_sem, 1)
        near_copy(slot).start()
        gather(mine, s, own_buf, slot)

        @pl.when(s >= 1)
        def _():
            near_copy(1 - slot).wait_recv()
            gather(other, s - 1, near_buf, 1 - slot)

        @pl.when(jnp.logical_and(s >= 1, s - 1 < steps - 2))
        def _():
            pl.semaphore_signal(free_sem, inc=1, device_id={'rows': near}, device_id_type=MESH)
        return carry
    lax.fori_loop(0, steps, step, 0)
    final = (steps - 1) % 2
    near_copy(final).wait_recv()
    gather(other, steps - 1, near_buf, final)

    def tile(j, t):
        begin = j * width + t * LANES
        return slice(begin, begin + LANES)

    def sweeps(phase, transposed, mass_row, mass_col, extra):
        def sends(slot, j):
            return [pltpu.make_async_remote_copy(
                src_ref=part_sum.at[phase, slot, j], dst_ref=peer_sum.at[phase, slot, k, j],
                send_sem=sum_send.at[phase, slot, k, j], recv_sem=sum_recv.at[phase, slot, k, j],
                device_id={'rows': peers[k]}, device_id_type=MESH) for k in range(GROUP - 1)]

        def top_sends(j):
            return [pltpu.make_async_remote_copy(
                src_ref=part_top.at[j], dst_ref=peer_top.at[k, j], send_sem=top_send.at[k, j],
                recv_sem=top_recv.at[k, j], device_id={'rows': peers[k]}, device_id_type=MESH) for k in range(GROUP - 1)]

        def row_update():
            for h in range(0, rows, 256):
                span = slice(h, h + 256)
                row_scale[span, :] = mass_row[span, :] / jnp.sum(row_acc[span, :], axis=1, keepdims=True)

        def col_pass(slot, j):
            def body(i, sums):
                span = pl.ds(i * BLOCK, BLOCK)
                scale = split(row_scale[span, :])
                return tuple(sums[t] + jnp.sum(split(acc[span, tile(j, t)]) * scale, axis=0) for t in range(tiles))
            sums = lax.fori_loop(0, rows // BLOCK, body, tuple(jnp.zeros((8, LANES), F32) for _ in range(tiles)))
            total = jnp.concatenate([jnp.sum(s, axis=0, keepdims=True) for s in sums], axis=0)
            if transposed:
                total = total * shift_fix[j]
            part_sum[phase, slot, j] = total
            for send in sends(slot, j):
                send.start()

        def col_update(slot, j):
            for send in sends(slot, j):
                send.wait()
            total = part_sum[phase, slot, j]
            for k in range(GROUP - 1):
                total = total + peer_sum[phase, slot, k, j]
            scale = mass_col[j] / total
            if transposed:
                scale = scale * shift_fix[j]
            col_scale[j] = scale

        def scale_rows(j):
            return [jnp.broadcast_to(col_scale[j, t:t + 1, :], (8, LANES)) for t in range(tiles)]

        def row_pass(j):
            scale = scale_rows(j)

            def body(i, carry):
                span = pl.ds(i * BLOCK, BLOCK)
                total = None if j == 0 else split(row_acc[span, :])
                for t in range(tiles):
                    term = split(acc[span, tile(j, t)]) * scale[t][None]
                    total = term if total is None else total + term
                row_acc[span, :] = total.reshape(BLOCK, LANES)
                return carry
            lax.fori_loop(0, rows // BLOCK, body, 0)

        if transposed:
            for j in range(CHUNKS):
                def top_block(i, tops, j=j):
                    span = pl.ds(i * BLOCK, BLOCK)
                    return tuple(jnp.maximum(tops[t], jnp.max(split(acc[span, tile(j, t)]), axis=0)) for t in range(tiles))
                tops = lax.fori_loop(0, rows // BLOCK, top_block, tuple(acc[0:8, tile(j, t)] for t in range(tiles)))
                tops = [jnp.max(top, axis=0, keepdims=True) for top in tops]
                wide = [jnp.broadcast_to(top, (8, LANES)) for top in tops]

                def exp_block(i, sums, j=j, wide=wide):
                    span = pl.ds(i * BLOCK, BLOCK)
                    out = []
                    for t in range(tiles):
                        val = jnp.exp((split(acc[span, tile(j, t)]) - wide[t][None]) * inv_eps)
                        acc[span, tile(j, t)] = val.reshape(BLOCK, LANES)
                        out.append(sums[t] + jnp.sum(val, axis=0))
                    return tuple(out)
                sums = lax.fori_loop(0, rows // BLOCK, exp_block, tuple(jnp.zeros((8, LANES), F32) for _ in range(tiles)))
                part_top[j, 0] = jnp.concatenate(tops, axis=0)
                part_top[j, 1] = jnp.concatenate([jnp.sum(s, axis=0, keepdims=True) for s in sums], axis=0)
                for send in top_sends(j):
                    send.start()
            for j in range(CHUNKS):
                for send in top_sends(j):
                    send.wait()
                top = part_top[j, 0]
                for k in range(GROUP - 1):
                    top = jnp.maximum(top, peer_top[k, j, 0])
                fix = jnp.exp((part_top[j, 0] - top) * inv_eps)
                total = part_top[j, 1] * fix
                for k in range(GROUP - 1):
                    total = total + peer_top[k, j, 1] * jnp.exp((peer_top[k, j, 0] - top) * inv_eps)
                shift_fix[j] = fix
                col_scale[j] = mass_col[j] / total * fix
                row_pass(j)
        else:
            def exp_rows(i, carry):
                span = pl.ds(i * BLOCK, BLOCK)
                top = acc[span, 0:LANES]
                for t in range(1, cols // LANES):
                    top = jnp.maximum(top, acc[span, t * LANES:(t + 1) * LANES])
                top = jnp.max(top, axis=1, keepdims=True)
                total = jnp.zeros((BLOCK, LANES), F32)
                for t in range(cols // LANES):
                    val = jnp.exp((acc[span, t * LANES:(t + 1) * LANES] - top) * inv_eps)
                    acc[span, t * LANES:(t + 1) * LANES] = val
                    total = total + val
                row_acc[span, :] = total
                return carry
            lax.fori_loop(0, rows // BLOCK, exp_rows, 0)
        row_update()

        def sweep(n, carry):
            slot = lax.rem(n, 2)
            for j in range(CHUNKS):
                col_pass(slot, j)
            extra(n)
            for j in range(CHUNKS):
                col_update(slot, j)
                row_pass(j)
            row_update()
            return carry
        if not transposed:
            extra(0)
        lax.fori_loop(0, SWEEPS - 1, sweep, 0)
        if transposed:
            for j in range(CHUNKS):
                scale = scale_rows(j)

                def plan_block(i, carry, j=j, scale=scale):
                    span = pl.ds(i * BLOCK, BLOCK)
                    left = split(row_scale[span, :])
                    for t in range(tiles):
                        val = left * split(acc[span, tile(j, t)]) * scale[t][None]
                        keep[span, tile(j, t)] = val.reshape(BLOCK, LANES).astype(BF16)
                    return carry
                lax.fori_loop(0, rows // BLOCK, plan_block, 0)
        else:
            for j in range(CHUNKS):
                col_pass((SWEEPS - 1) % 2, j)
            for j in range(CHUNKS):
                col_update((SWEEPS - 1) % 2, j)

    def late(n):
        for index, copy in enumerate(late_pieces):
            pl.when(n == index)(copy.start)

    for copy in mass_out:
        copy.wait_recv()
    sweeps(0, True, mass_rows_t, mass_all, late)

    order = [(k, h) for k in (2, 3, 1, 0) for h in range(per)]

    def src_again(n):
        return pltpu.make_async_copy(rows_of(src, src_near, src_far, *order[n]), src_buf.at[n % 2], src_sem.at[n % 2])

    column = aligned(me * rows, rows)
    a_copies, own_stores = [], []
    src_again(0).start()
    for n, (k, h) in enumerate(order):
        src_again(n).wait()
        if n + 1 < len(order):
            src_again(n + 1).start()

        def make(t, carry, n=n):
            span = aligned(t * 256, 256)
            made[n, :, span] = mm(src_buf[n % 2], keep[span, :], NT).astype(BF16)
            return carry
        lax.fori_loop(0, rows // 256, make, 0)
        target = ready.at[pl.ds(h * SLAB, SLAB), column]
        if k:
            a_copies.append(remote(made.at[n], target, devices[k], reserve(1)))
            a_copies[-1].start()
        else:
            own_stores.append(pltpu.make_async_copy(made.at[n], target, block_sem.at[h]))
            own_stores[-1].start()

    tgt_feat_near.wait_recv()
    tgt_feat_out.wait_recv()
    tgt_feat_pass.start()
    for copy in tgt_out:
        copy.wait_recv()
    tgt_pass.start()
    tgt_near_out.wait_recv()
    tgt_feat_pass.wait_recv()
    cross_terms(feat_src, lambda k: feat_tgt if k == 0 else tgt_feat_peer.at[k - 1])
    tgt_pass.wait_recv()
    for store in own_stores:
        store.wait()
    assemble(tgt, tgt_near, tgt_blocks, tgt_far, slab, turned, block_sem, chip, core, rows)

    def tgt_load(n):
        return pltpu.make_async_copy(rows_of(tgt, tgt_near, tgt_far, *ordered[n]), src_buf.at[n % 2], src_sem.at[n % 2])

    def left_load(n):
        k, h = ordered[n]
        return pltpu.make_async_copy(ready.at[:, aligned(devices[k] * rows + h * SLAB, SLAB)], left_buf.at[n % 2],
                                     load_sem.at[n % 2])

    def prepare(n):
        k, h = ordered[n]
        if k and h == 0:
            for copy, (kk, hh) in zip(a_copies, order):
                if kk == k:
                    copy.wait_recv()
        tgt_load(n).start()
        left_load(n).start()

    prepare(0)
    for n, (k, h) in enumerate(ordered):
        tgt_load(n).wait()
        left_load(n).wait()
        if n + 1 < len(ordered) and not (k and h == per - 1):
            prepare(n + 1)

        def update(t, carry, n=n):
            span = aligned(t * TILE, TILE)
            acc[:, span] += weighted(mm(left_buf[n % 2], src_buf[n % 2, :, span], NN), 2.0 * (1.0 - ALPHA))
            return carry
        lax.fori_loop(0, cols // TILE, update, 0)
        if n + 1 < len(ordered) and k and h == per - 1:
            prepare(n + 1)

    kern_store = pltpu.make_async_copy(acc, kern_out, load_sem.at[2])

    def store_kernel(n):
        if isinstance(n, int):
            kern_store.start()
    sweeps(1, False, mass_rows, mass_cols, store_kernel)
    row_out[...] = row_scale[...]
    col_out[...] = col_scale[...]
    kern_store.wait()
    for slot in range(2):
        near_copy(slot).wait_send()
    for copy in ([src_near_out, src_feat_near, start_near_out, tgt_near_out, tgt_feat_near, src_feat_out, tgt_feat_out,
                  src_pass, src_feat_pass, tgt_pass, tgt_feat_pass] + src_out + tgt_out + mass_out + a_copies):
        copy.wait_send()
    for s in range(steps):
        for copy in start_out(s):
            copy.wait_send()


def solution(mesh):
    def local_fgw(cost_src, cost_tgt, plan_init, mass_src, mass_tgt, feat_src, feat_tgt, epsilon):
        rows, cols = cost_src.shape
        half, quad = cols // 2, rows // 2
        depth = feat_src.shape[1]
        tiles = cols // LANES // CHUNKS
        me = lax.axis_index('rows')
        mass_cols_mine = lax.dynamic_slice(mass_tgt, (rows * me,), (rows,))
        vec = (CHUNKS, tiles, LANES)
        n_links = 31 + 2 * (half // STEP) + 2 + 3 * rows // SLAB
        any_spec = pl.BlockSpec(memory_space=pl.ANY)
        vmem_spec = pl.BlockSpec(memory_space=pltpu.VMEM)
        hbm = [((rows, cols), BF16), ((rows, cols), BF16),
               ((rows, cols), BF16), ((2, 5, quad, quad), BF16), ((half, cols), BF16),
               ((rows, cols), BF16), ((2, 5, quad, quad), BF16), ((half, cols), BF16),
               ((GROUP - 1, rows, depth), BF16), ((GROUP - 1, rows, depth), BF16),
               ((rows, half), BF16), ((2, rows, half), BF16), ((rows, cols), BF16)]
        outs = [((rows, cols), F32), ((rows, LANES), F32), (vec, F32)] + hbm
        vmem = [((rows, cols), F32), ((rows, cols), BF16), ((2, SLAB, cols), BF16), ((cols, STEP), BF16),
                ((2, cols, STEP), BF16), ((2, cols, STEP), BF16), ((GROUP * rows // SLAB, SLAB, rows), BF16),
                ((2, rows, SLAB), BF16), ((SLAB, half), BF16), ((half, SLAB), BF16), ((2, rows, depth), BF16),
                (vec, F32), ((rows, LANES), F32), ((rows, LANES), F32), (vec, F32), (vec, F32),
                ((2, 2) + vec, F32), ((2, 2, GROUP - 1) + vec, F32),
                ((CHUNKS, 2, tiles, LANES), F32), ((GROUP - 1, CHUNKS, 2, tiles, LANES), F32)]
        sems = [(6,), (2,), (15,), (n_links,), (n_links,), (2, 2, GROUP - 1, CHUNKS), (2, 2, GROUP - 1, CHUNKS),
                (GROUP - 1, CHUNKS), (GROUP - 1, CHUNKS)]
        result = pl.pallas_call(
            kernel,
            out_shape=[jax.ShapeDtypeStruct(*s) for s in outs],
            in_specs=[any_spec] * 5 + [vmem_spec] * 4 + [pl.BlockSpec(memory_space=pltpu.SMEM)],
            out_specs=[any_spec, vmem_spec, vmem_spec] + [any_spec] * len(hbm),
            scratch_shapes=[pltpu.VMEM(*s) for s in vmem] + [pltpu.SemaphoreType.DMA(s) for s in sems]
            + [pltpu.SemaphoreType.REGULAR],
            compiler_params=pltpu.CompilerParams(collective_id=0, has_side_effects=True, vmem_limit_bytes=67000000),
            cost_estimate=pl.CostEstimate(flops=10 * rows * cols * cols, bytes_accessed=700000000,
                                          transcendentals=2 * rows * cols),
            name='fused_gw',
        )(cost_src, cost_tgt, plan_init.astype(BF16), feat_src.astype(BF16), feat_tgt.astype(BF16),
          mass_src.reshape(tiles, LANES), jnp.broadcast_to(mass_cols_mine[:, None], (rows, LANES)),
          jnp.broadcast_to(mass_src[:, None], (rows, LANES)), mass_tgt.reshape(vec), epsilon.reshape(1))
        kern, row_scale, col_scale = result[:3]
        return row_scale[:, :1] * kern * col_scale.reshape(1, cols)

    row_spec = P(('pairs', 'rows'), None)
    vec_spec = P(('pairs', 'rows'))
    in_specs = (row_spec, row_spec, row_spec, vec_spec, P('pairs'), row_spec, row_spec, P())
    return jax.shard_map(local_fgw, mesh=mesh, in_specs=in_specs, out_specs=row_spec, check_vma=False)
```

```python
import functools

import jax
import jax.numpy as jnp
from jax import lax
from jax.experimental import pallas as pl
from jax.experimental.pallas import tpu as pltpu
from jax.sharding import PartitionSpec as P

ALPHA = 0.5
SWEEPS = 10
LANES = 128
CHUNKS = 4
BLOCK = 64
STEP = 256
SLAB = 512
TILE = 512
EARLY_STEPS = 1
TAIL_PIECES = 4
GROUP = 4
PART = 256
SPLIT = 4
MESH = pl.DeviceIdType.MESH
NT = (((1,), (1,)), ((), ()))
NN = (((1,), (0,)), ((), ()))
BF16 = jnp.bfloat16
F32 = jnp.float32


def weighted(value, factor):
    return value if factor == 1.0 else value * factor


def mm(left, right, dims):
    return lax.dot_general(left, right, dims, preferred_element_type=F32)


class Copies:
    def __init__(self, source, target, sems, rows):
        part = rows // SPLIT
        self.parts = [pltpu.make_async_copy(source.at[pl.ds(i * part, part)], target.at[pl.ds(i * part, part)], sems.at[i])
                      for i in range(SPLIT)]

    def start(self):
        for part in self.parts:
            part.start()

    def wait(self):
        for part in self.parts:
            part.wait()


def split(val):
    return val.reshape(val.shape[0] // 8, 8, LANES)


def aligned(start, size):
    return pl.ds(pl.multiple_of(start, size), size)


def turn_corner(cost, cost_near, far, slab, turned, sems, chip, core, rows):
    half = 2 * rows
    away = half * (1 - chip)
    for source, owner in ((cost, core), (cost_near, 1 - core)):
        for a in range(rows // SLAB):
            load = pltpu.make_async_copy(source.at[pl.ds(a * SLAB, SLAB), aligned(away, half)], slab, sems.at[0])
            load.start()
            load.wait()

            def turn(b, carry):
                turned[aligned(b * SLAB, SLAB), :] = slab[:, aligned(b * SLAB, SLAB)].T
                return carry
            lax.fori_loop(0, half // SLAB, turn, 0)
            store = pltpu.make_async_copy(turned, far.at[:, aligned(half * chip + owner * rows + a * SLAB, SLAB)], sems.at[1])
            store.start()
            store.wait()


def place_corner(blocks, far, slab, turned, sems, chip, core, rows):
    quad = rows // 2
    half = 2 * rows
    away = half * (1 - chip)

    def corner(k, carry):
        cc = core + k - 2 * core * k
        base, other = cc * rows, (1 - cc) * rows
        spots = [(base, base), (base, base + quad), (base + quad, base + quad),
                 (base, other + quad * cc), (base + quad * cc, other + quad)]
        loads = [pltpu.make_async_copy(blocks.at[k, b], slab.at[:, pl.ds(b * quad, quad)] if b < 4 else
                                       turned.at[pl.ds(3 * quad, quad), :], sems.at[2 + b]) for b in range(5)]
        for load in loads:
            load.start()
        for load in loads:
            load.wait()
        turned[pl.ds(0, quad), :] = slab[:, quad:2 * quad].T
        turned[pl.ds(quad, quad), :] = slab[:, 3 * quad:4 * quad].T
        turned[pl.ds(2 * quad, quad), :] = turned[pl.ds(3 * quad, quad), :].T
        stores = []

        def put(source, row, col):
            target = far.at[aligned(row, quad), aligned(away + col, quad)]
            stores.append(pltpu.make_async_copy(source, target, sems.at[7 + len(stores)]))
            stores[-1].start()
        for b in range(4):
            put(slab.at[:, pl.ds(b * quad, quad)], *spots[b])
        put(turned.at[pl.ds(3 * quad, quad), :], *spots[4])
        for t, b in enumerate((1, 3, 4)):
            put(turned.at[pl.ds(t * quad, quad), :], spots[b][1], spots[b][0])
        for store in stores:
            store.wait()
        return carry
    lax.fori_loop(0, 2, corner, 0)


def kernel(src_f32, tgt_f32, start, feat_src, feat_tgt, mass_mine, mass_rows_t, mass_rows, mass_cols, epsilon,
           kern_out, row_out, col_out, src, tgt, src_near, src_blocks, src_far, tgt_near, tgt_blocks, tgt_far,
           src_feat_peer, tgt_feat_peer, start_near, start_far, ready,
           acc, keep, src_buf, start_buf, own_buf, near_buf, made, left_buf, slab, turned, feat_buf, mass_all,
           row_scale, row_acc, col_scale, shift_fix, part_sum, peer_sum, part_top, peer_top,
           load_sem, src_sem, block_sem, send_sem, recv_sem, sum_send, sum_recv, top_send, top_recv, free_sem):
    rows, cols = src_f32.shape
    half = cols // 2
    quad = rows // 2
    steps = half // STEP
    per = rows // SLAB
    tiles = cols // LANES // CHUNKS
    width = cols // CHUNKS
    me = lax.axis_index('rows')
    chip, core = me // 2, me % 2
    near, same, cross = chip * 2 + (1 - core), (1 - chip) * 2 + core, (1 - chip) * 2 + (1 - core)
    peers = (near, same, cross)
    devices = (me, near, same, cross)
    inv_eps = 1.0 / epsilon[0]

    src_load_all = [pltpu.make_async_copy(src_f32.at[pl.ds(b * quad, quad)], acc.at[pl.ds(b * quad, quad)], load_sem.at[b])
                    for b in range(2)]
    for load in src_load_all:
        load.start()
    mass_all[me] = mass_mine[...]
    barrier = pltpu.get_barrier_semaphore()
    for peer in peers:
        pl.semaphore_signal(barrier, inc=1, device_id={'rows': peer}, device_id_type=MESH)
    pl.semaphore_wait(barrier, GROUP - 1)

    counter = [0]

    def reserve(count):
        counter[0] += count
        return counter[0] - count

    def remote(source, target, peer, index):
        return pltpu.make_async_remote_copy(src_ref=source, dst_ref=target, send_sem=send_sem.at[index],
                                            recv_sem=recv_sem.at[index], device_id={'rows': peer}, device_id_type=MESH)

    def col_span(base, s):
        return aligned(base + s * STEP, STEP)

    def block_spots():
        diag, off = me * rows, (me + 1 - 2 * core) * rows
        return [(0, diag), (0, diag + quad), (quad, diag + quad), (0, off + quad * core), (quad * core, off + quad)]

    mine, other = half * core, half * (1 - core)
    src_near_out = remote(src, src_near, near, reserve(1))
    src_feat_near = remote(feat_src, src_feat_peer.at[0], near, reserve(1))
    start_near_out = remote(start.at[:, aligned(other, half)], start_near, near, reserve(1))
    tgt_near_out = remote(tgt, tgt_near, near, reserve(1))
    tgt_feat_near = remote(feat_tgt, tgt_feat_peer.at[0], near, reserve(1))
    src_out = [remote(src.at[aligned(row, quad), aligned(col, quad)], src_blocks.at[0, b], same, reserve(1))
               for b, (row, col) in enumerate(block_spots())]
    src_feat_out = remote(feat_src, src_feat_peer.at[1], same, reserve(1))
    tgt_feat_out = remote(feat_tgt, tgt_feat_peer.at[1], same, reserve(1))
    piece = quad // 2
    tgt_out = [remote(tgt.at[aligned(row + h * piece, piece), aligned(col, quad)],
                      tgt_blocks.at[0, b, pl.ds(h * piece, piece)], same, reserve(1))
               for b, (row, col) in enumerate(block_spots()) for h in range(2)]
    src_pass = remote(src_blocks.at[0], src_blocks.at[1], near, reserve(1))
    src_feat_pass = remote(src_feat_peer.at[1], src_feat_peer.at[2], near, reserve(1))
    tgt_pass = remote(tgt_blocks.at[0], tgt_blocks.at[1], near, reserve(1))
    tgt_feat_pass = remote(tgt_feat_peer.at[1], tgt_feat_peer.at[2], near, reserve(1))
    mass_out = [remote(mass_mine, mass_all.at[me], peer, reserve(1)) for peer in peers]
    start_base = reserve(2 * steps)
    near_base = reserve(2)
    late_pieces = tgt_out[TAIL_PIECES:] + [tgt_feat_out]

    def start_out(s):
        return [remote(start.at[:, col_span(mine, s)], start_far.at[0, :, col_span(0, s)], same, start_base + s),
                remote(start.at[:, col_span(other, s)], start_far.at[1, :, col_span(0, s)], cross, start_base + steps + s)]

    def near_copy(slot):
        return remote(own_buf.at[slot], near_buf.at[slot], near, near_base + slot)

    for s in range(EARLY_STEPS):
        for copy in start_out(s):
            copy.start()
    for copy in [start_near_out, src_feat_near, tgt_feat_near] + mass_out:
        copy.start()

    src_stores = []
    for b in range(2):
        src_load_all[b].wait()

        def cast(t, carry, b=b):
            span = aligned(t * BLOCK, BLOCK)
            src_buf[b, span, :] = acc[aligned(b * quad + t * BLOCK, BLOCK), :].astype(BF16)
            return carry
        lax.fori_loop(0, quad // BLOCK, cast, 0)
        src_stores.append(pltpu.make_async_copy(src_buf.at[b], src.at[pl.ds(b * quad, quad)], src_sem.at[b, 0]))
        src_stores[-1].start()
    tgt_load_all = pltpu.make_async_copy(tgt_f32, acc, load_sem.at[0])
    tgt_load_all.start()
    for store in src_stores:
        store.wait()
    for copy in [src_feat_out, src_near_out] + src_out:
        copy.start()
    for s in range(EARLY_STEPS, steps):
        for copy in start_out(s):
            copy.start()
    tgt_load_all.wait()

    def cast_tgt(t, carry):
        span = aligned(t * BLOCK, BLOCK)
        keep[span, :] = acc[span, :].astype(BF16)
        return carry
    lax.fori_loop(0, rows // BLOCK, cast_tgt, 0)
    tgt_store = pltpu.make_async_copy(keep, tgt, load_sem.at[0])
    tgt_store.start()
    tgt_store.wait()
    tgt_near_out.start()
    for copy in tgt_out[:TAIL_PIECES]:
        copy.start()

    def cross_terms(first, peer_second):
        depth = feat_buf.shape[1]
        seconds = [left_buf.at[k // 2, :, pl.ds(k % 2 * depth, depth)] for k in range(GROUP)]
        loads = [pltpu.make_async_copy(first, feat_buf, load_sem.at[1])]
        loads += [pltpu.make_async_copy(peer_second(k), seconds[k], load_sem.at[2 + k]) for k in range(GROUP)]
        for load in loads:
            load.start()
        for load in loads:
            load.wait()
        for k, device in enumerate(devices):

            def cross_term(h, carry, device=device, k=k):
                second = left_buf[k // 2, aligned(h * TILE, TILE), k % 2 * depth:(k % 2 + 1) * depth]
                acc[:, aligned(device * rows + h * TILE, TILE)] = weighted(mm(feat_buf[...], second, NT), 2.0 * ALPHA)
                return carry
            lax.fori_loop(0, rows // TILE, cross_term, 0)

    src_near_out.wait_recv()
    turn_corner(src, src_near, src_far, slab, turned, block_sem, chip, core, rows)
    src_feat_near.wait_recv()
    src_feat_out.wait_recv()
    src_feat_pass.start()
    src_feat_pass.wait_recv()
    cross_terms(feat_tgt, lambda k: feat_src if k == 0 else src_feat_peer.at[k - 1])
    tgt_near_out.wait_recv()
    turn_corner(tgt, tgt_near, tgt_far, slab, turned, block_sem, chip, core, rows)
    for copy in src_out:
        copy.wait_recv()
    src_pass.start()
    src_pass.wait_recv()
    place_corner(src_blocks, src_far, slab, turned, block_sem, chip, core, rows)

    def rows_of(matrix, matrix_near, matrix_far, k, h):
        if k == 0:
            return matrix.at[pl.ds(h * SLAB, SLAB)]
        if k == 1:
            return matrix_near.at[pl.ds(h * SLAB, SLAB)]
        which = core if k == 2 else 1 - core
        return matrix_far.at[aligned(which * rows + h * SLAB, SLAB)]

    ordered = [(k, h) for k in range(GROUP) for h in range(per)]

    def src_load(b):
        return Copies(rows_of(src, src_near, src_far, *ordered[b]), src_buf.at[b % 2], src_sem.at[b % 2], SLAB)

    def gather(parts):
        def update(h, carry):
            span = aligned(h * TILE, TILE)
            left = [keep[:, col_span(base, s)] for base, s, _, _ in parts]
            right = [buf[slot, span, :] for _, _, buf, slot in parts]
            block = mm(jnp.concatenate(left, axis=1), jnp.concatenate(right, axis=1), NT)
            acc[:, span] += weighted(block, 2.0 * (1.0 - ALPHA))
            return carry
        lax.fori_loop(0, cols // TILE, update, 0, unroll=2)

    start_near_out.wait_recv()
    src_load(0).start()

    def step(s, carry):
        slot = lax.rem(s, 2)
        for copy in start_out(s):
            copy.wait_recv()
        loads = []
        for k, device in enumerate(devices):
            source = (start.at[:, col_span(mine, s)] if k == 0 else start_near.at[:, col_span(0, s)] if k == 1
                      else start_far.at[k - 2, :, col_span(0, s)])
            landing = turned.at[pl.ds(k // 2 * rows, rows), pl.ds(k % 2 * STEP, STEP)]
            loads.append(pltpu.make_async_copy(source, landing, load_sem.at[2 + k]))
        for load in loads:
            load.start()

        @pl.when(s >= 2)
        def _():
            near_copy(slot).wait_send()
        for k, load in enumerate(loads):
            load.wait()

            def turn(t, carry, k=k):
                block = turned[aligned(k // 2 * rows + t * STEP, STEP), pl.ds(k % 2 * STEP, STEP)]
                start_buf[:, aligned(devices[k] * rows + t * STEP, STEP)] = block.T
                return carry
            lax.fori_loop(0, rows // STEP, turn, 0, unroll=2)
        for b, (k, h) in enumerate(ordered):
            src_load(b).wait()
            if b + 1 < len(ordered):
                src_load(b + 1).start()
            else:
                @pl.when(s + 1 < steps)
                def _():
                    src_load(0).start()

            def part_a(t, carry, b=b, k=k, h=h):
                value = mm(src_buf[b % 2, aligned(t * PART, PART), :], start_buf[...], NT).astype(BF16)
                own_buf[slot, aligned(devices[k] * rows + h * SLAB + t * PART, PART), :] = value
                return carry
            lax.fori_loop(0, SLAB // PART, part_a, 0)

        @pl.when(s >= 2)
        def _():
            pl.semaphore_wait(free_sem, 1)
        near_copy(slot).start()

        @pl.when(s == 0)
        def _():
            gather([(mine, s, own_buf, slot)])

        @pl.when(s >= 1)
        def _():
            near_copy(1 - slot).wait_recv()
            gather([(mine, s, own_buf, slot), (other, s - 1, near_buf, 1 - slot)])

        @pl.when(jnp.logical_and(s >= 1, s - 1 < steps - 2))
        def _():
            pl.semaphore_signal(free_sem, inc=1, device_id={'rows': near}, device_id_type=MESH)
        return carry
    lax.fori_loop(0, steps, step, 0)
    final = (steps - 1) % 2
    near_copy(final).wait_recv()
    gather([(other, steps - 1, near_buf, final)])

    def tile(j, t):
        begin = j * width + t * LANES
        return slice(begin, begin + LANES)

    def sweeps(phase, transposed, mass_row, mass_col, extra):
        def sends(slot, j):
            return [pltpu.make_async_remote_copy(
                src_ref=part_sum.at[phase, slot, j], dst_ref=peer_sum.at[phase, slot, k, j],
                send_sem=sum_send.at[phase, slot, k, j], recv_sem=sum_recv.at[phase, slot, k, j],
                device_id={'rows': peers[k]}, device_id_type=MESH) for k in range(GROUP - 1)]

        def top_sends(j):
            return [pltpu.make_async_remote_copy(
                src_ref=part_top.at[j], dst_ref=peer_top.at[k, j], send_sem=top_send.at[k, j],
                recv_sem=top_recv.at[k, j], device_id={'rows': peers[k]}, device_id_type=MESH) for k in range(GROUP - 1)]

        def row_update():
            for h in range(0, rows, 256):
                span = slice(h, h + 256)
                row_scale[span, :] = mass_row[span, :] / jnp.sum(row_acc[span, :], axis=1, keepdims=True)

        def col_pass(slot, j):
            def body(i, sums):
                span = pl.ds(i * BLOCK, BLOCK)
                scale = split(row_scale[span, :])
                return tuple(sums[t] + jnp.sum(split(acc[span, tile(j, t)]) * scale, axis=0) for t in range(tiles))
            sums = lax.fori_loop(0, rows // BLOCK, body, tuple(jnp.zeros((8, LANES), F32) for _ in range(tiles)), unroll=2)
            total = jnp.concatenate([jnp.sum(s, axis=0, keepdims=True) for s in sums], axis=0)
            if transposed:
                total = total * shift_fix[j]
            part_sum[phase, slot, j] = total
            for send in sends(slot, j):
                send.start()

        def col_update(slot, j):
            for send in sends(slot, j):
                send.wait()
            total = part_sum[phase, slot, j]
            for k in range(GROUP - 1):
                total = total + peer_sum[phase, slot, k, j]
            scale = mass_col[j] / total
            if transposed:
                scale = scale * shift_fix[j]
            col_scale[j] = scale

        def scale_rows(j):
            return [jnp.broadcast_to(col_scale[j, t:t + 1, :], (8, LANES)) for t in range(tiles)]

        def row_pass(j):
            scale = scale_rows(j)

            def body(i, carry):
                span = pl.ds(i * BLOCK, BLOCK)
                total = None if j == 0 else split(row_acc[span, :])
                for t in range(tiles):
                    term = split(acc[span, tile(j, t)]) * scale[t][None]
                    total = term if total is None else total + term
                row_acc[span, :] = total.reshape(BLOCK, LANES)
                return carry
            lax.fori_loop(0, rows // BLOCK, body, 0, unroll=2)

        if transposed:
            for j in range(CHUNKS):
                def top_block(i, tops, j=j):
                    span = pl.ds(i * BLOCK, BLOCK)
                    return tuple(jnp.maximum(tops[t], jnp.max(split(acc[span, tile(j, t)]), axis=0)) for t in range(tiles))
                tops = lax.fori_loop(0, rows // BLOCK, top_block, tuple(acc[0:8, tile(j, t)] for t in range(tiles)))
                tops = [jnp.max(top, axis=0, keepdims=True) for top in tops]
                wide = [jnp.broadcast_to(top, (8, LANES)) for top in tops]

                def exp_block(i, sums, j=j, wide=wide):
                    span = pl.ds(i * BLOCK, BLOCK)
                    out = []
                    for t in range(tiles):
                        val = jnp.exp((split(acc[span, tile(j, t)]) - wide[t][None]) * inv_eps)
                        acc[span, tile(j, t)] = val.reshape(BLOCK, LANES)
                        out.append(sums[t] + jnp.sum(val, axis=0))
                    return tuple(out)
                sums = lax.fori_loop(0, rows // BLOCK, exp_block, tuple(jnp.zeros((8, LANES), F32) for _ in range(tiles)))
                part_top[j, 0] = jnp.concatenate(tops, axis=0)
                part_top[j, 1] = jnp.concatenate([jnp.sum(s, axis=0, keepdims=True) for s in sums], axis=0)
                for send in top_sends(j):
                    send.start()
            for j in range(CHUNKS):
                for send in top_sends(j):
                    send.wait()
                top = part_top[j, 0]
                for k in range(GROUP - 1):
                    top = jnp.maximum(top, peer_top[k, j, 0])
                fix = jnp.exp((part_top[j, 0] - top) * inv_eps)
                total = part_top[j, 1] * fix
                for k in range(GROUP - 1):
                    total = total + peer_top[k, j, 1] * jnp.exp((peer_top[k, j, 0] - top) * inv_eps)
                shift_fix[j] = fix
                col_scale[j] = mass_col[j] / total * fix
                row_pass(j)
        else:
            def exp_rows(i, carry):
                span = pl.ds(i * BLOCK, BLOCK)
                top = acc[span, 0:LANES]
                for t in range(1, cols // LANES):
                    top = jnp.maximum(top, acc[span, t * LANES:(t + 1) * LANES])
                top = jnp.max(top, axis=1, keepdims=True)
                total = jnp.zeros((BLOCK, LANES), F32)
                for t in range(cols // LANES):
                    val = jnp.exp((acc[span, t * LANES:(t + 1) * LANES] - top) * inv_eps)
                    acc[span, t * LANES:(t + 1) * LANES] = val
                    total = total + val
                row_acc[span, :] = total
                return carry
            lax.fori_loop(0, rows // BLOCK, exp_rows, 0)
        row_update()

        def sweep(n, carry):
            slot = lax.rem(n, 2)
            for j in range(CHUNKS):
                col_pass(slot, j)
            extra(n)
            for j in range(CHUNKS):
                col_update(slot, j)
                row_pass(j)
            row_update()
            return carry
        if not transposed:
            extra(0)
        lax.fori_loop(0, SWEEPS - 1, sweep, 0)
        if transposed:
            for j in range(CHUNKS):
                scale = scale_rows(j)

                def plan_block(i, carry, j=j, scale=scale):
                    span = pl.ds(i * BLOCK, BLOCK)
                    left = split(row_scale[span, :])
                    for t in range(tiles):
                        val = left * split(acc[span, tile(j, t)]) * scale[t][None]
                        keep[span, tile(j, t)] = val.reshape(BLOCK, LANES).astype(BF16)
                    return carry
                lax.fori_loop(0, rows // BLOCK, plan_block, 0)
        else:
            for j in range(CHUNKS):
                col_pass((SWEEPS - 1) % 2, j)
            for j in range(CHUNKS):
                col_update((SWEEPS - 1) % 2, j)

    def late(n):
        for index, copy in enumerate(late_pieces):
            pl.when(n == index)(copy.start)

    for copy in mass_out:
        copy.wait_recv()
    sweeps(0, True, mass_rows_t, mass_all, late)

    order = [(k, h) for k in (2, 3, 1, 0) for h in range(per)]

    def src_again(n):
        return Copies(rows_of(src, src_near, src_far, *order[n]), src_buf.at[n % 2], src_sem.at[n % 2], SLAB)

    column = aligned(me * rows, rows)
    a_copies, own_stores = [], []
    src_again(0).start()
    for n, (k, h) in enumerate(order):
        src_again(n).wait()
        if n + 1 < len(order):
            src_again(n + 1).start()

        def make(t, carry, n=n):
            span = aligned(t * 256, 256)
            made[n, :, span] = mm(src_buf[n % 2], keep[span, :], NT).astype(BF16)
            return carry
        lax.fori_loop(0, rows // 256, make, 0, unroll=2)
        target = ready.at[pl.ds(h * SLAB, SLAB), column]
        if k:
            a_copies.append(remote(made.at[n], target, devices[k], reserve(1)))
            a_copies[-1].start()
        else:
            own_stores.append(pltpu.make_async_copy(made.at[n], target, block_sem.at[h]))
            own_stores[-1].start()

    tgt_feat_near.wait_recv()
    tgt_feat_out.wait_recv()
    tgt_feat_pass.start()
    for copy in tgt_out:
        copy.wait_recv()
    tgt_pass.start()
    tgt_feat_pass.wait_recv()
    cross_terms(feat_src, lambda k: feat_tgt if k == 0 else tgt_feat_peer.at[k - 1])
    tgt_pass.wait_recv()
    for store in own_stores:
        store.wait()
    place_corner(tgt_blocks, tgt_far, slab, turned, block_sem, chip, core, rows)

    def tgt_load(n):
        return Copies(rows_of(tgt, tgt_near, tgt_far, *ordered[n]), src_buf.at[n % 2], src_sem.at[n % 2], SLAB)

    def left_load(n):
        k, h = ordered[n]
        return pltpu.make_async_copy(ready.at[:, aligned(devices[k] * rows + h * SLAB, SLAB)], left_buf.at[n % 2],
                                     load_sem.at[n % 2])

    def prepare(n):
        k, h = ordered[n]
        if k and h == 0:
            for copy, (kk, hh) in zip(a_copies, order):
                if kk == k:
                    copy.wait_recv()
        tgt_load(n).start()
        left_load(n).start()

    prepare(0)
    for n, (k, h) in enumerate(ordered):
        tgt_load(n).wait()
        left_load(n).wait()
        if n + 1 < len(ordered) and not (k and h == per - 1):
            prepare(n + 1)

        def update(t, carry, n=n):
            span = aligned(t * TILE, TILE)
            acc[:, span] += weighted(mm(left_buf[n % 2], src_buf[n % 2, :, span], NN), 2.0 * (1.0 - ALPHA))
            return carry
        lax.fori_loop(0, cols // TILE, update, 0, unroll=2)
        if n + 1 < len(ordered) and k and h == per - 1:
            prepare(n + 1)

    kern_store = pltpu.make_async_copy(acc, kern_out, load_sem.at[2])

    def store_kernel(n):
        if isinstance(n, int):
            kern_store.start()
    sweeps(1, False, mass_rows, mass_cols, store_kernel)
    row_out[...] = row_scale[...]
    col_out[...] = col_scale[...]
    kern_store.wait()
    for slot in range(2):
        near_copy(slot).wait_send()
    for copy in ([src_near_out, src_feat_near, start_near_out, tgt_near_out, tgt_feat_near, src_feat_out, tgt_feat_out,
                  src_pass, src_feat_pass, tgt_pass, tgt_feat_pass] + src_out + tgt_out + mass_out + a_copies):
        copy.wait_send()
    for s in range(steps):
        for copy in start_out(s):
            copy.wait_send()


def solution(mesh):
    def local_fgw(cost_src, cost_tgt, plan_init, mass_src, mass_tgt, feat_src, feat_tgt, epsilon):
        rows, cols = cost_src.shape
        half, quad = cols // 2, rows // 2
        depth = feat_src.shape[1]
        tiles = cols // LANES // CHUNKS
        me = lax.axis_index('rows')
        mass_cols_mine = lax.dynamic_slice(mass_tgt, (rows * me,), (rows,))
        vec = (CHUNKS, tiles, LANES)
        n_links = 31 + 2 * (half // STEP) + 2 + 3 * rows // SLAB
        any_spec = pl.BlockSpec(memory_space=pl.ANY)
        vmem_spec = pl.BlockSpec(memory_space=pltpu.VMEM)
        hbm = [((rows, cols), BF16), ((rows, cols), BF16),
               ((rows, cols), BF16), ((2, 5, quad, quad), BF16), ((half, cols), BF16),
               ((rows, cols), BF16), ((2, 5, quad, quad), BF16), ((half, cols), BF16),
               ((GROUP - 1, rows, depth), BF16), ((GROUP - 1, rows, depth), BF16),
               ((rows, half), BF16), ((2, rows, half), BF16), ((rows, cols), BF16)]
        outs = [((rows, cols), F32), ((rows, LANES), F32), (vec, F32)] + hbm
        vmem = [((rows, cols), F32), ((rows, cols), BF16), ((2, SLAB, cols), BF16), ((STEP, cols), BF16),
                ((2, cols, STEP), BF16), ((2, cols, STEP), BF16), ((GROUP * rows // SLAB, SLAB, rows), BF16),
                ((2, rows, SLAB), BF16), ((SLAB, half), BF16), ((half, SLAB), BF16), ((rows, depth), BF16),
                (vec, F32), ((rows, LANES), F32), ((rows, LANES), F32), (vec, F32), (vec, F32),
                ((2, 2) + vec, F32), ((2, 2, GROUP - 1) + vec, F32),
                ((CHUNKS, 2, tiles, LANES), F32), ((GROUP - 1, CHUNKS, 2, tiles, LANES), F32)]
        sems = [(6,), (2, SPLIT), (15,), (n_links,), (n_links,), (2, 2, GROUP - 1, CHUNKS), (2, 2, GROUP - 1, CHUNKS),
                (GROUP - 1, CHUNKS), (GROUP - 1, CHUNKS)]
        result = pl.pallas_call(
            kernel,
            out_shape=[jax.ShapeDtypeStruct(*s) for s in outs],
            in_specs=[any_spec] * 5 + [vmem_spec] * 4 + [pl.BlockSpec(memory_space=pltpu.SMEM)],
            out_specs=[any_spec, vmem_spec, vmem_spec] + [any_spec] * len(hbm),
            scratch_shapes=[pltpu.VMEM(*s) for s in vmem] + [pltpu.SemaphoreType.DMA(s) for s in sems]
            + [pltpu.SemaphoreType.REGULAR],
            compiler_params=pltpu.CompilerParams(collective_id=0, has_side_effects=True, vmem_limit_bytes=67000000),
            cost_estimate=pl.CostEstimate(flops=10 * rows * cols * cols, bytes_accessed=700000000,
                                          transcendentals=2 * rows * cols),
            name='fused_gw',
        )(cost_src, cost_tgt, plan_init.astype(BF16), feat_src.astype(BF16), feat_tgt.astype(BF16),
          mass_src.reshape(tiles, LANES), jnp.broadcast_to(mass_cols_mine[:, None], (rows, LANES)),
          jnp.broadcast_to(mass_src[:, None], (rows, LANES)), mass_tgt.reshape(vec), epsilon.reshape(1))
        kern, row_scale, col_scale = result[:3]
        return row_scale[:, :1] * kern * col_scale.reshape(1, cols)

    row_spec = P(('pairs', 'rows'), None)
    vec_spec = P(('pairs', 'rows'))
    in_specs = (row_spec, row_spec, row_spec, vec_spec, P('pairs'), row_spec, row_spec, P())
    return jax.shard_map(local_fgw, mesh=mesh, in_specs=in_specs, out_specs=row_spec, check_vma=False)
```

```python
import functools

import jax
import jax.numpy as jnp
from jax import lax
from jax.experimental import pallas as pl
from jax.experimental.pallas import tpu as pltpu
from jax.sharding import PartitionSpec as P

ALPHA = 0.5
SWEEPS = 10
LANES = 128
CHUNKS = 4
BLOCK = 64
STEP = 256
SLAB = 512
TILE = 512
TAIL_PIECES = 7
GROUP = 4
PART = 256
SPLIT = 4
MESH = pl.DeviceIdType.MESH
NT = (((1,), (1,)), ((), ()))
NN = (((1,), (0,)), ((), ()))
BF16 = jnp.bfloat16
F32 = jnp.float32


def weighted(value, factor):
    return value if factor == 1.0 else value * factor


def mm(left, right, dims):
    return lax.dot_general(left, right, dims, preferred_element_type=F32)


class Copies:
    def __init__(self, source, target, sems, rows):
        part = rows // SPLIT
        self.parts = [pltpu.make_async_copy(source.at[pl.ds(i * part, part)], target.at[pl.ds(i * part, part)], sems.at[i])
                      for i in range(SPLIT)]

    def start(self):
        for part in self.parts:
            part.start()

    def wait(self):
        for part in self.parts:
            part.wait()


def split(val):
    return val.reshape(val.shape[0] // 8, 8, LANES)


def aligned(start, size):
    return pl.ds(pl.multiple_of(start, size), size)


def turn_corner(cost, cost_near, far, slab, turned, sems, chip, core, rows):
    half = 2 * rows
    away = half * (1 - chip)
    for source, owner in ((cost, core), (cost_near, 1 - core)):
        for a in range(rows // SLAB):
            load = pltpu.make_async_copy(source.at[pl.ds(a * SLAB, SLAB), aligned(away, half)], slab, sems.at[0])
            load.start()
            load.wait()

            def turn(b, carry):
                turned[aligned(b * SLAB, SLAB), :] = slab[:, aligned(b * SLAB, SLAB)].T
                return carry
            lax.fori_loop(0, half // SLAB, turn, 0)
            store = pltpu.make_async_copy(turned, far.at[:, aligned(half * chip + owner * rows + a * SLAB, SLAB)], sems.at[1])
            store.start()
            store.wait()


def place_corner(blocks, far, slab, turned, sems, chip, core, rows):
    quad = rows // 2
    half = 2 * rows
    away = half * (1 - chip)

    def corner(k, carry):
        cc = core + k - 2 * core * k
        base, other = cc * rows, (1 - cc) * rows
        spots = [(base, base), (base, base + quad), (base + quad, base + quad),
                 (base, other + quad * cc), (base + quad * cc, other + quad)]
        loads = [pltpu.make_async_copy(blocks.at[k, b], slab.at[:, pl.ds(b * quad, quad)] if b < 4 else
                                       turned.at[pl.ds(3 * quad, quad), :], sems.at[2 + b]) for b in range(5)]
        for load in loads:
            load.start()
        for load in loads:
            load.wait()
        turned[pl.ds(0, quad), :] = slab[:, quad:2 * quad].T
        turned[pl.ds(quad, quad), :] = slab[:, 3 * quad:4 * quad].T
        turned[pl.ds(2 * quad, quad), :] = turned[pl.ds(3 * quad, quad), :].T
        stores = []

        def put(source, row, col):
            target = far.at[aligned(row, quad), aligned(away + col, quad)]
            stores.append(pltpu.make_async_copy(source, target, sems.at[7 + len(stores)]))
            stores[-1].start()
        for b in range(4):
            put(slab.at[:, pl.ds(b * quad, quad)], *spots[b])
        put(turned.at[pl.ds(3 * quad, quad), :], *spots[4])
        for t, b in enumerate((1, 3, 4)):
            put(turned.at[pl.ds(t * quad, quad), :], spots[b][1], spots[b][0])
        for store in stores:
            store.wait()
        return carry
    lax.fori_loop(0, 2, corner, 0)


def kernel(src_f32, tgt_f32, start_f32, feat_src_f32, feat_tgt_f32, mass_mine, mass_rows_t, mass_rows, mass_cols, epsilon,
           kern_out, row_out, col_out, start, feat_src, feat_tgt, src, tgt, src_near, src_blocks, src_far, tgt_near, tgt_blocks, tgt_far,
           src_feat_peer, tgt_feat_peer, start_near, start_far, ready,
           acc, keep, src_buf, start_buf, own_buf, near_buf, made, left_buf, slab, turned, feat_buf, mass_all,
           row_scale, row_acc, col_scale, shift_fix, part_sum, peer_sum, part_top, peer_top,
           load_sem, src_sem, block_sem, send_sem, recv_sem, sum_send, sum_recv, top_send, top_recv, free_sem):
    rows, cols = src_f32.shape
    half = cols // 2
    quad = rows // 2
    steps = half // STEP
    per = rows // SLAB
    tiles = cols // LANES // CHUNKS
    width = cols // CHUNKS
    me = lax.axis_index('rows')
    chip, core = me // 2, me % 2
    near, same, cross = chip * 2 + (1 - core), (1 - chip) * 2 + core, (1 - chip) * 2 + (1 - core)
    peers = (near, same, cross)
    devices = (me, near, same, cross)
    inv_eps = 1.0 / epsilon[0]

    src_load_all = [pltpu.make_async_copy(src_f32.at[pl.ds(b * quad, quad)], acc.at[pl.ds(b * quad, quad)], load_sem.at[b])
                    for b in range(2)]
    mine, other = half * core, half * (1 - core)
    depth = feat_src_f32.shape[1]

    def col_span(base, s):
        return aligned(base + s * STEP, STEP)

    heads = [(start_f32.at[:, col_span(mine, 0)], start.at[:, col_span(mine, 0)], STEP),
             (start_f32.at[:, col_span(other, 0)], start.at[:, col_span(other, 0)], STEP),
             (feat_src_f32, feat_src, depth), (feat_tgt_f32, feat_tgt, depth)]
    head_loads, head_stores = [], []
    for n, (source, target, size) in enumerate(heads):
        head_loads.append(pltpu.make_async_copy(source, acc.at[:, pl.ds(n * size, size)], load_sem.at[2 + n]))
        head_loads[-1].start()
        head_stores.append(pltpu.make_async_copy(left_buf.at[n // 2, :, pl.ds(n % 2 * size, size)], target, load_sem.at[2 + n]))
    mass_all[me] = mass_mine[...]
    barrier = pltpu.get_barrier_semaphore()
    for peer in peers:
        pl.semaphore_signal(barrier, inc=1, device_id={'rows': peer}, device_id_type=MESH)
    pl.semaphore_wait(barrier, GROUP - 1)

    counter = [0]

    def reserve(count):
        counter[0] += count
        return counter[0] - count

    def remote(source, target, peer, index):
        return pltpu.make_async_remote_copy(src_ref=source, dst_ref=target, send_sem=send_sem.at[index],
                                            recv_sem=recv_sem.at[index], device_id={'rows': peer}, device_id_type=MESH)

    def block_spots():
        diag, off = me * rows, (me + 1 - 2 * core) * rows
        return [(0, diag), (0, diag + quad), (quad, diag + quad), (0, off + quad * core), (quad * core, off + quad)]

    src_near_out = remote(src, src_near, near, reserve(1))
    src_feat_near = remote(feat_src, src_feat_peer.at[0], near, reserve(1))
    start_near_out = remote(start.at[:, aligned(other, half)], start_near, near, reserve(1))
    tgt_near_out = remote(tgt, tgt_near, near, reserve(1))
    tgt_feat_near = remote(feat_tgt, tgt_feat_peer.at[0], near, reserve(1))
    src_out = [remote(src.at[aligned(row, quad), aligned(col, quad)], src_blocks.at[0, b], same, reserve(1))
               for b, (row, col) in enumerate(block_spots())]
    src_feat_out = remote(feat_src, src_feat_peer.at[1], same, reserve(1))
    tgt_feat_out = remote(feat_tgt, tgt_feat_peer.at[1], same, reserve(1))
    piece = quad // 2
    tgt_out = [remote(tgt.at[aligned(row + h * piece, piece), aligned(col, quad)],
                      tgt_blocks.at[0, b, pl.ds(h * piece, piece)], same, reserve(1))
               for b, (row, col) in enumerate(block_spots()) for h in range(2)]
    src_pass = remote(src_blocks.at[0], src_blocks.at[1], near, reserve(1))
    src_feat_pass = remote(src_feat_peer.at[1], src_feat_peer.at[2], near, reserve(1))
    tgt_pass = remote(tgt_blocks.at[0], tgt_blocks.at[1], near, reserve(1))
    tgt_feat_pass = remote(tgt_feat_peer.at[1], tgt_feat_peer.at[2], near, reserve(1))
    mass_out = [remote(mass_mine, mass_all.at[me], peer, reserve(1)) for peer in peers]
    start_base = reserve(2 * steps)
    near_base = reserve(2)
    late_pieces = tgt_out[TAIL_PIECES:] + [tgt_feat_out]

    def start_out(s):
        return [remote(start.at[:, col_span(mine, s)], start_far.at[0, :, col_span(0, s)], same, start_base + s),
                remote(start.at[:, col_span(other, s)], start_far.at[1, :, col_span(0, s)], cross, start_base + steps + s)]

    def near_copy(slot):
        return remote(own_buf.at[slot], near_buf.at[slot], near, near_base + slot)

    for n, (_, _, size) in enumerate(heads):
        head_loads[n].wait()

        def cast_head(t, carry, n=n, size=size):
            span = aligned(t * 256, 256)
            left_buf[n // 2, span, n % 2 * size:(n % 2 + 1) * size] = acc[span, n * size:(n + 1) * size].astype(BF16)
            return carry
        lax.fori_loop(0, rows // 256, cast_head, 0)
        head_stores[n].start()
    for load in src_load_all:
        load.start()
    for store in head_stores:
        store.wait()
    for copy in start_out(0):
        copy.start()
    for copy in [src_feat_near, tgt_feat_near] + mass_out:
        copy.start()

    src_stores = []
    for b in range(2):
        src_load_all[b].wait()

        def cast(t, carry, b=b):
            span = aligned(t * BLOCK, BLOCK)
            src_buf[b, span, :] = acc[aligned(b * quad + t * BLOCK, BLOCK), :].astype(BF16)
            return carry
        lax.fori_loop(0, quad // BLOCK, cast, 0)
        src_stores.append(pltpu.make_async_copy(src_buf.at[b], src.at[pl.ds(b * quad, quad)], src_sem.at[b, 0]))
        src_stores[-1].start()
    start_load = pltpu.make_async_copy(start_f32, acc, load_sem.at[0])
    start_load.start()
    for store in src_stores:
        store.wait()
    for copy in [src_feat_out, src_near_out] + src_out:
        copy.start()

    def cast_keep(t, carry):
        span = aligned(t * BLOCK, BLOCK)
        keep[span, :] = acc[span, :].astype(BF16)
        return carry
    start_load.wait()
    lax.fori_loop(0, rows // BLOCK, cast_keep, 0)
    tgt_load_all = pltpu.make_async_copy(tgt_f32, acc, load_sem.at[0])
    tgt_load_all.start()
    rest = half - STEP
    start_stores = []
    for n, base in enumerate((mine, other)):
        span = pl.ds(pl.multiple_of(base + STEP, STEP), rest)
        start_stores.append(pltpu.make_async_copy(keep.at[:, span], start.at[:, span], load_sem.at[2 + n]))
        start_stores[-1].start()
    for store in start_stores:
        store.wait()
    for s in range(1, steps):
        for copy in start_out(s):
            copy.start()
    start_near_out.start()
    tgt_load_all.wait()
    lax.fori_loop(0, rows // BLOCK, cast_keep, 0)
    tgt_store = pltpu.make_async_copy(keep, tgt, load_sem.at[0])
    tgt_store.start()
    tgt_store.wait()
    tgt_near_out.start()
    for copy in tgt_out[:TAIL_PIECES]:
        copy.start()

    def cross_terms(first, peer_second):
        depth = feat_buf.shape[1]
        seconds = [left_buf.at[k // 2, :, pl.ds(k % 2 * depth, depth)] for k in range(GROUP)]
        loads = [pltpu.make_async_copy(first, feat_buf, load_sem.at[1])]
        loads += [pltpu.make_async_copy(peer_second(k), seconds[k], load_sem.at[2 + k]) for k in range(GROUP)]
        for load in loads:
            load.start()
        for load in loads:
            load.wait()
        for k, device in enumerate(devices):

            def cross_term(h, carry, device=device, k=k):
                second = left_buf[k // 2, aligned(h * TILE, TILE), k % 2 * depth:(k % 2 + 1) * depth]
                acc[:, aligned(device * rows + h * TILE, TILE)] = weighted(mm(feat_buf[...], second, NT), 2.0 * ALPHA)
                return carry
            lax.fori_loop(0, rows // TILE, cross_term, 0)

    src_near_out.wait_recv()
    turn_corner(src, src_near, src_far, slab, turned, block_sem, chip, core, rows)
    src_feat_near.wait_recv()
    src_feat_out.wait_recv()
    src_feat_pass.start()
    src_feat_pass.wait_recv()
    cross_terms(feat_tgt, lambda k: feat_src if k == 0 else src_feat_peer.at[k - 1])
    tgt_near_out.wait_recv()
    turn_corner(tgt, tgt_near, tgt_far, slab, turned, block_sem, chip, core, rows)
    for copy in src_out:
        copy.wait_recv()
    src_pass.start()
    src_pass.wait_recv()
    place_corner(src_blocks, src_far, slab, turned, block_sem, chip, core, rows)

    def rows_of(matrix, matrix_near, matrix_far, k, h):
        if k == 0:
            return matrix.at[pl.ds(h * SLAB, SLAB)]
        if k == 1:
            return matrix_near.at[pl.ds(h * SLAB, SLAB)]
        which = core if k == 2 else 1 - core
        return matrix_far.at[aligned(which * rows + h * SLAB, SLAB)]

    ordered = [(k, h) for k in range(GROUP) for h in range(per)]

    def src_load(b):
        return Copies(rows_of(src, src_near, src_far, *ordered[b]), src_buf.at[b % 2], src_sem.at[b % 2], SLAB)

    def gather(parts):
        def update(h, carry):
            span = aligned(h * TILE, TILE)
            left = [keep[:, col_span(base, s)] for base, s, _, _ in parts]
            right = [buf[slot, span, :] for _, _, buf, slot in parts]
            block = mm(jnp.concatenate(left, axis=1), jnp.concatenate(right, axis=1), NT)
            acc[:, span] += weighted(block, 2.0 * (1.0 - ALPHA))
            return carry
        lax.fori_loop(0, cols // TILE, update, 0, unroll=2)

    start_near_out.wait_recv()
    src_load(0).start()

    def step(s, carry):
        slot = lax.rem(s, 2)
        for copy in start_out(s):
            copy.wait_recv()
        loads = []
        for k, device in enumerate(devices):
            source = (start.at[:, col_span(mine, s)] if k == 0 else start_near.at[:, col_span(0, s)] if k == 1
                      else start_far.at[k - 2, :, col_span(0, s)])
            landing = turned.at[pl.ds(k // 2 * rows, rows), pl.ds(k % 2 * STEP, STEP)]
            loads.append(pltpu.make_async_copy(source, landing, load_sem.at[2 + k]))
        for load in loads:
            load.start()

        @pl.when(s >= 2)
        def _():
            near_copy(slot).wait_send()
        for k, load in enumerate(loads):
            load.wait()

            def turn(t, carry, k=k):
                block = turned[aligned(k // 2 * rows + t * STEP, STEP), pl.ds(k % 2 * STEP, STEP)]
                start_buf[:, aligned(devices[k] * rows + t * STEP, STEP)] = block.T
                return carry
            lax.fori_loop(0, rows // STEP, turn, 0, unroll=2)
        for b, (k, h) in enumerate(ordered):
            src_load(b).wait()
            if b + 1 < len(ordered):
                src_load(b + 1).start()
            else:
                @pl.when(s + 1 < steps)
                def _():
                    src_load(0).start()

            def part_a(t, carry, b=b, k=k, h=h):
                value = mm(src_buf[b % 2, aligned(t * PART, PART), :], start_buf[...], NT).astype(BF16)
                own_buf[slot, aligned(devices[k] * rows + h * SLAB + t * PART, PART), :] = value
                return carry
            lax.fori_loop(0, SLAB // PART, part_a, 0, unroll=2)

        @pl.when(s >= 2)
        def _():
            pl.semaphore_wait(free_sem, 1)
        near_copy(slot).start()

        @pl.when(s == 0)
        def _():
            gather([(mine, s, own_buf, slot)])

        @pl.when(s >= 1)
        def _():
            near_copy(1 - slot).wait_recv()
            gather([(mine, s, own_buf, slot), (other, s - 1, near_buf, 1 - slot)])

        @pl.when(jnp.logical_and(s >= 1, s - 1 < steps - 2))
        def _():
            pl.semaphore_signal(free_sem, inc=1, device_id={'rows': near}, device_id_type=MESH)
        return carry
    lax.fori_loop(0, steps, step, 0)
    final = (steps - 1) % 2
    near_copy(final).wait_recv()
    gather([(other, steps - 1, near_buf, final)])

    def tile(j, t):
        begin = j * width + t * LANES
        return slice(begin, begin + LANES)

    def sweeps(phase, transposed, mass_row, mass_col, extra):
        def sends(slot, j):
            return [pltpu.make_async_remote_copy(
                src_ref=part_sum.at[phase, slot, j], dst_ref=peer_sum.at[phase, slot, k, j],
                send_sem=sum_send.at[phase, slot, k, j], recv_sem=sum_recv.at[phase, slot, k, j],
                device_id={'rows': peers[k]}, device_id_type=MESH) for k in range(GROUP - 1)]

        def top_sends(j):
            return [pltpu.make_async_remote_copy(
                src_ref=part_top.at[j], dst_ref=peer_top.at[k, j], send_sem=top_send.at[k, j],
                recv_sem=top_recv.at[k, j], device_id={'rows': peers[k]}, device_id_type=MESH) for k in range(GROUP - 1)]

        def row_update():
            for h in range(0, rows, 256):
                span = slice(h, h + 256)
                row_scale[span, :] = mass_row[span, :] / jnp.sum(row_acc[span, :], axis=1, keepdims=True)

        def col_pass(slot, j):
            def body(i, sums):
                span = pl.ds(i * BLOCK, BLOCK)
                scale = split(row_scale[span, :])
                return tuple(sums[t] + jnp.sum(split(acc[span, tile(j, t)]) * scale, axis=0) for t in range(tiles))
            sums = lax.fori_loop(0, rows // BLOCK, body, tuple(jnp.zeros((8, LANES), F32) for _ in range(tiles)), unroll=2)
            total = jnp.concatenate([jnp.sum(s, axis=0, keepdims=True) for s in sums], axis=0)
            if transposed:
                total = total * shift_fix[j]
            part_sum[phase, slot, j] = total
            for send in sends(slot, j):
                send.start()

        def col_update(slot, j):
            for send in sends(slot, j):
                send.wait()
            total = part_sum[phase, slot, j]
            for k in range(GROUP - 1):
                total = total + peer_sum[phase, slot, k, j]
            scale = mass_col[j] / total
            if transposed:
                scale = scale * shift_fix[j]
            col_scale[j] = scale

        def scale_rows(j):
            return [jnp.broadcast_to(col_scale[j, t:t + 1, :], (8, LANES)) for t in range(tiles)]

        def row_pass(j):
            scale = scale_rows(j)

            def body(i, carry):
                span = pl.ds(i * BLOCK, BLOCK)
                total = None if j == 0 else split(row_acc[span, :])
                for t in range(tiles):
                    term = split(acc[span, tile(j, t)]) * scale[t][None]
                    total = term if total is None else total + term
                row_acc[span, :] = total.reshape(BLOCK, LANES)
                return carry
            lax.fori_loop(0, rows // BLOCK, body, 0, unroll=2)

        if transposed:
            for j in range(CHUNKS):
                def top_block(i, tops, j=j):
                    span = pl.ds(i * BLOCK, BLOCK)
                    return tuple(jnp.maximum(tops[t], jnp.max(split(acc[span, tile(j, t)]), axis=0)) for t in range(tiles))
                tops = lax.fori_loop(0, rows // BLOCK, top_block, tuple(acc[0:8, tile(j, t)] for t in range(tiles)))
                tops = [jnp.max(top, axis=0, keepdims=True) for top in tops]
                wide = [jnp.broadcast_to(top, (8, LANES)) for top in tops]

                def exp_block(i, sums, j=j, wide=wide):
                    span = pl.ds(i * BLOCK, BLOCK)
                    out = []
                    for t in range(tiles):
                        val = jnp.exp((split(acc[span, tile(j, t)]) - wide[t][None]) * inv_eps)
                        acc[span, tile(j, t)] = val.reshape(BLOCK, LANES)
                        out.append(sums[t] + jnp.sum(val, axis=0))
                    return tuple(out)
                sums = lax.fori_loop(0, rows // BLOCK, exp_block, tuple(jnp.zeros((8, LANES), F32) for _ in range(tiles)))
                part_top[j, 0] = jnp.concatenate(tops, axis=0)
                part_top[j, 1] = jnp.concatenate([jnp.sum(s, axis=0, keepdims=True) for s in sums], axis=0)
                for send in top_sends(j):
                    send.start()
            for j in range(CHUNKS):
                for send in top_sends(j):
                    send.wait()
                top = part_top[j, 0]
                for k in range(GROUP - 1):
                    top = jnp.maximum(top, peer_top[k, j, 0])
                fix = jnp.exp((part_top[j, 0] - top) * inv_eps)
                total = part_top[j, 1] * fix
                for k in range(GROUP - 1):
                    total = total + peer_top[k, j, 1] * jnp.exp((peer_top[k, j, 0] - top) * inv_eps)
                shift_fix[j] = fix
                col_scale[j] = mass_col[j] / total * fix
                row_pass(j)
        else:
            def exp_rows(i, carry):
                span = pl.ds(i * BLOCK, BLOCK)
                top = acc[span, 0:LANES]
                for t in range(1, cols // LANES):
                    top = jnp.maximum(top, acc[span, t * LANES:(t + 1) * LANES])
                top = jnp.max(top, axis=1, keepdims=True)
                total = jnp.zeros((BLOCK, LANES), F32)
                for t in range(cols // LANES):
                    val = jnp.exp((acc[span, t * LANES:(t + 1) * LANES] - top) * inv_eps)
                    acc[span, t * LANES:(t + 1) * LANES] = val
                    total = total + val
                row_acc[span, :] = total
                return carry
            lax.fori_loop(0, rows // BLOCK, exp_rows, 0)
        row_update()

        def sweep(n, carry):
            slot = lax.rem(n, 2)
            for j in range(CHUNKS):
                col_pass(slot, j)
            extra(n)
            for j in range(CHUNKS):
                col_update(slot, j)
                row_pass(j)
            row_update()
            return carry
        if not transposed:
            extra(0)
        lax.fori_loop(0, SWEEPS - 1, sweep, 0)
        if transposed:
            for j in range(CHUNKS):
                scale = scale_rows(j)

                def plan_block(i, carry, j=j, scale=scale):
                    span = pl.ds(i * BLOCK, BLOCK)
                    left = split(row_scale[span, :])
                    for t in range(tiles):
                        val = left * split(acc[span, tile(j, t)]) * scale[t][None]
                        keep[span, tile(j, t)] = val.reshape(BLOCK, LANES).astype(BF16)
                    return carry
                lax.fori_loop(0, rows // BLOCK, plan_block, 0)
        else:
            for j in range(CHUNKS):
                col_pass((SWEEPS - 1) % 2, j)
            for j in range(CHUNKS):
                col_update((SWEEPS - 1) % 2, j)

    def late(n):
        for index, copy in enumerate(late_pieces):
            pl.when(n == index)(copy.start)

    for copy in mass_out:
        copy.wait_recv()
    sweeps(0, True, mass_rows_t, mass_all, late)

    order = [(k, h) for k in (2, 3, 1, 0) for h in range(per)]

    def src_again(n):
        return Copies(rows_of(src, src_near, src_far, *order[n]), src_buf.at[n % 2], src_sem.at[n % 2], SLAB)

    column = aligned(me * rows, rows)
    a_copies, own_stores = [], []
    src_again(0).start()
    for n, (k, h) in enumerate(order):
        src_again(n).wait()
        if n + 1 < len(order):
            src_again(n + 1).start()

        def make(t, carry, n=n):
            span = aligned(t * 256, 256)
            made[n, :, span] = mm(src_buf[n % 2], keep[span, :], NT).astype(BF16)
            return carry
        lax.fori_loop(0, rows // 256, make, 0, unroll=2)
        target = ready.at[pl.ds(h * SLAB, SLAB), column]
        if k:
            a_copies.append(remote(made.at[n], target, devices[k], reserve(1)))
            a_copies[-1].start()
        else:
            own_stores.append(pltpu.make_async_copy(made.at[n], target, block_sem.at[h]))
            own_stores[-1].start()

    tgt_feat_near.wait_recv()
    tgt_feat_out.wait_recv()
    tgt_feat_pass.start()
    for copy in tgt_out:
        copy.wait_recv()
    tgt_pass.start()
    tgt_feat_pass.wait_recv()
    cross_terms(feat_src, lambda k: feat_tgt if k == 0 else tgt_feat_peer.at[k - 1])
    tgt_pass.wait_recv()
    for store in own_stores:
        store.wait()
    place_corner(tgt_blocks, tgt_far, slab, turned, block_sem, chip, core, rows)

    def stage(k):
        if k % 2 == 0:
            return [src_buf.at[h] for h in range(per)], [left_buf.at[h] for h in range(per)]
        return [keep.at[pl.ds(h * SLAB, SLAB)] for h in range(per)], [turned.at[pl.ds(h * rows, rows)] for h in range(per)]

    def tgt_loads(k):
        return [Copies(rows_of(tgt, tgt_near, tgt_far, k, h), stage(k)[0][h], src_sem.at[k % 2 * per + h], SLAB)
                for h in range(per)]

    def left_loads(k):
        return [pltpu.make_async_copy(ready.at[:, aligned(devices[k] * rows + h * SLAB, SLAB)], stage(k)[1][h],
                                      load_sem.at[k % 2 * per + h]) for h in range(per)]

    def begin_left(k):
        for copy, (kk, _) in zip(a_copies, order):
            if kk == k:
                copy.wait_recv()
        for load in left_loads(k):
            load.start()

    for load in tgt_loads(0):
        load.start()
    begin_left(0)
    for k in range(GROUP):
        if k + 1 < GROUP:
            for load in tgt_loads(k + 1):
                load.start()
        if k + 1 < GROUP - 1:
            begin_left(k + 1)
        elif k == GROUP - 1:
            begin_left(k)
        for load in tgt_loads(k) + left_loads(k):
            load.wait()
        rights, lefts = stage(k)

        def update(t, carry, rights=rights, lefts=lefts):
            span = aligned(t * TILE, TILE)
            total = mm(lefts[0][...], rights[0][:, span], NN)
            for h in range(1, per):
                total = total + mm(lefts[h][...], rights[h][:, span], NN)
            acc[:, span] += weighted(total, 2.0 * (1.0 - ALPHA))
            return carry
        lax.fori_loop(0, cols // TILE, update, 0)

    kern_store = pltpu.make_async_copy(acc, kern_out, load_sem.at[2])

    def store_kernel(n):
        if isinstance(n, int):
            kern_store.start()
    sweeps(1, False, mass_rows, mass_cols, store_kernel)
    row_out[...] = row_scale[...]
    col_out[...] = col_scale[...]
    kern_store.wait()
    for slot in range(2):
        near_copy(slot).wait_send()
    for copy in ([src_near_out, src_feat_near, start_near_out, tgt_near_out, tgt_feat_near, src_feat_out, tgt_feat_out,
                  src_pass, src_feat_pass, tgt_pass, tgt_feat_pass] + src_out + tgt_out + mass_out + a_copies):
        copy.wait_send()
    for s in range(steps):
        for copy in start_out(s):
            copy.wait_send()


def solution(mesh):
    def local_fgw(cost_src, cost_tgt, plan_init, mass_src, mass_tgt, feat_src, feat_tgt, epsilon):
        rows, cols = cost_src.shape
        half, quad = cols // 2, rows // 2
        depth = feat_src.shape[1]
        tiles = cols // LANES // CHUNKS
        me = lax.axis_index('rows')
        mass_cols_mine = lax.dynamic_slice(mass_tgt, (rows * me,), (rows,))
        vec = (CHUNKS, tiles, LANES)
        n_links = 31 + 2 * (half // STEP) + 2 + 3 * rows // SLAB
        any_spec = pl.BlockSpec(memory_space=pl.ANY)
        vmem_spec = pl.BlockSpec(memory_space=pltpu.VMEM)
        hbm = [((rows, cols), BF16), ((rows, depth), BF16), ((rows, depth), BF16),
               ((rows, cols), BF16), ((rows, cols), BF16),
               ((rows, cols), BF16), ((2, 5, quad, quad), BF16), ((half, cols), BF16),
               ((rows, cols), BF16), ((2, 5, quad, quad), BF16), ((half, cols), BF16),
               ((GROUP - 1, rows, depth), BF16), ((GROUP - 1, rows, depth), BF16),
               ((rows, half), BF16), ((2, rows, half), BF16), ((rows, cols), BF16)]
        outs = [((rows, cols), F32), ((rows, LANES), F32), (vec, F32)] + hbm
        vmem = [((rows, cols), F32), ((rows, cols), BF16), ((2, SLAB, cols), BF16), ((STEP, cols), BF16),
                ((2, cols, STEP), BF16), ((2, cols, STEP), BF16), ((GROUP * rows // SLAB, SLAB, rows), BF16),
                ((2, rows, SLAB), BF16), ((SLAB, half), BF16), ((half, SLAB), BF16), ((rows, depth), BF16),
                (vec, F32), ((rows, LANES), F32), ((rows, LANES), F32), (vec, F32), (vec, F32),
                ((2, 2) + vec, F32), ((2, 2, GROUP - 1) + vec, F32),
                ((CHUNKS, 2, tiles, LANES), F32), ((GROUP - 1, CHUNKS, 2, tiles, LANES), F32)]
        sems = [(8,), (4, SPLIT), (15,), (n_links,), (n_links,), (2, 2, GROUP - 1, CHUNKS), (2, 2, GROUP - 1, CHUNKS),
                (GROUP - 1, CHUNKS), (GROUP - 1, CHUNKS)]
        result = pl.pallas_call(
            kernel,
            out_shape=[jax.ShapeDtypeStruct(*s) for s in outs],
            in_specs=[any_spec] * 5 + [vmem_spec] * 4 + [pl.BlockSpec(memory_space=pltpu.SMEM)],
            out_specs=[any_spec, vmem_spec, vmem_spec] + [any_spec] * len(hbm),
            scratch_shapes=[pltpu.VMEM(*s) for s in vmem] + [pltpu.SemaphoreType.DMA(s) for s in sems]
            + [pltpu.SemaphoreType.REGULAR],
            compiler_params=pltpu.CompilerParams(collective_id=0, has_side_effects=True, vmem_limit_bytes=67000000),
            cost_estimate=pl.CostEstimate(flops=10 * rows * cols * cols, bytes_accessed=700000000,
                                          transcendentals=2 * rows * cols),
            name='fused_gw',
        )(cost_src, cost_tgt, plan_init, feat_src, feat_tgt,
          mass_src.reshape(tiles, LANES), jnp.broadcast_to(mass_cols_mine[:, None], (rows, LANES)),
          jnp.broadcast_to(mass_src[:, None], (rows, LANES)), mass_tgt.reshape(vec), epsilon.reshape(1))
        kern, row_scale, col_scale = result[:3]
        return row_scale[:, :1] * kern * col_scale.reshape(1, cols)

    row_spec = P(('pairs', 'rows'), None)
    vec_spec = P(('pairs', 'rows'))
    in_specs = (row_spec, row_spec, row_spec, vec_spec, P('pairs'), row_spec, row_spec, P())
    return jax.shard_map(local_fgw, mesh=mesh, in_specs=in_specs, out_specs=row_spec, check_vma=False)
```

```python
import functools

import jax
import jax.numpy as jnp
from jax import lax
from jax.experimental import pallas as pl
from jax.experimental.pallas import tpu as pltpu
from jax.sharding import PartitionSpec as P

ALPHA = 0.5
SWEEPS = 10
LANES = 128
CHUNKS = 4
BLOCK = 64
STEP = 256
SLAB = 512
TILE = 512
TAIL_PIECES = 16
PIECES = 4
GROUP = 4
PART = 256
SPLIT = 4
MESH = pl.DeviceIdType.MESH
NT = (((1,), (1,)), ((), ()))
NN = (((1,), (0,)), ((), ()))
BF16 = jnp.bfloat16
F32 = jnp.float32


def weighted(value, factor):
    return value if factor == 1.0 else value * factor


def mm(left, right, dims):
    return lax.dot_general(left, right, dims, preferred_element_type=F32)


class Copies:
    def __init__(self, source, target, sems, rows):
        part = rows // SPLIT
        self.parts = [pltpu.make_async_copy(source.at[pl.ds(i * part, part)], target.at[pl.ds(i * part, part)], sems.at[i])
                      for i in range(SPLIT)]

    def start(self):
        for part in self.parts:
            part.start()

    def wait(self):
        for part in self.parts:
            part.wait()


def split(val):
    return val.reshape(val.shape[0] // 8, 8, LANES)


def aligned(start, size):
    return pl.ds(pl.multiple_of(start, size), size)


def turn_corner(cost, cost_near, far, slab, turned, sems, chip, core, rows):
    half = 2 * rows
    away = half * (1 - chip)
    for source, owner in ((cost, core), (cost_near, 1 - core)):
        for a in range(rows // SLAB):
            load = pltpu.make_async_copy(source.at[pl.ds(a * SLAB, SLAB), aligned(away, half)], slab, sems.at[0])
            load.start()
            load.wait()

            def turn(b, carry):
                turned[aligned(b * SLAB, SLAB), :] = slab[:, aligned(b * SLAB, SLAB)].T
                return carry
            lax.fori_loop(0, half // SLAB, turn, 0)
            store = pltpu.make_async_copy(turned, far.at[:, aligned(half * chip + owner * rows + a * SLAB, SLAB)], sems.at[1])
            store.start()
            store.wait()


def place_corner(blocks, far, slab, turned, sems, chip, core, rows):
    quad = rows // 2
    half = 2 * rows
    away = half * (1 - chip)

    def corner(k, carry):
        cc = core + k - 2 * core * k
        base, other = cc * rows, (1 - cc) * rows
        spots = [(base, base), (base, base + quad), (base + quad, base + quad),
                 (base, other + quad * cc), (base + quad * cc, other + quad)]
        loads = [pltpu.make_async_copy(blocks.at[k, b], slab.at[:, pl.ds(b * quad, quad)] if b < 4 else
                                       turned.at[pl.ds(3 * quad, quad), :], sems.at[2 + b]) for b in range(5)]
        for load in loads:
            load.start()
        for load in loads:
            load.wait()
        turned[pl.ds(0, quad), :] = slab[:, quad:2 * quad].T
        turned[pl.ds(quad, quad), :] = slab[:, 3 * quad:4 * quad].T
        turned[pl.ds(2 * quad, quad), :] = turned[pl.ds(3 * quad, quad), :].T
        stores = []

        def put(source, row, col):
            target = far.at[aligned(row, quad), aligned(away + col, quad)]
            stores.append(pltpu.make_async_copy(source, target, sems.at[7 + len(stores)]))
            stores[-1].start()
        for b in range(4):
            put(slab.at[:, pl.ds(b * quad, quad)], *spots[b])
        put(turned.at[pl.ds(3 * quad, quad), :], *spots[4])
        for t, b in enumerate((1, 3, 4)):
            put(turned.at[pl.ds(t * quad, quad), :], spots[b][1], spots[b][0])
        for store in stores:
            store.wait()
        return carry
    lax.fori_loop(0, 2, corner, 0)


def kernel(src_f32, tgt_f32, start_f32, feat_src_f32, feat_tgt_f32, mass_mine, mass_rows_t, mass_rows, mass_cols, epsilon,
           kern_out, row_out, col_out, start, feat_src, feat_tgt, src, tgt, src_near, src_blocks, src_far, tgt_near, tgt_blocks, tgt_far,
           src_feat_peer, tgt_feat_peer, start_near, start_far, ready,
           acc, keep, src_buf, start_buf, own_buf, near_buf, made, left_buf, slab, turned, feat_buf, mass_all,
           row_scale, row_acc, col_scale, shift_fix, part_sum, peer_sum, part_top, peer_top,
           load_sem, src_sem, block_sem, send_sem, recv_sem, sum_send, sum_recv, top_send, top_recv, free_sem):
    rows, cols = src_f32.shape
    half = cols // 2
    quad = rows // 2
    steps = half // STEP
    per = rows // SLAB
    tiles = cols // LANES // CHUNKS
    width = cols // CHUNKS
    me = lax.axis_index('rows')
    chip, core = me // 2, me % 2
    near, same, cross = chip * 2 + (1 - core), (1 - chip) * 2 + core, (1 - chip) * 2 + (1 - core)
    peers = (near, same, cross)
    devices = (me, near, same, cross)
    inv_eps = 1.0 / epsilon[0]

    src_load_all = [pltpu.make_async_copy(src_f32.at[pl.ds(b * quad, quad)], acc.at[pl.ds(b * quad, quad)], load_sem.at[b])
                    for b in range(2)]
    mine, other = half * core, half * (1 - core)
    depth = feat_src_f32.shape[1]

    def col_span(base, s):
        return aligned(base + s * STEP, STEP)

    heads = [(start_f32.at[:, col_span(mine, 0)], start.at[:, col_span(mine, 0)], STEP),
             (start_f32.at[:, col_span(other, 0)], start.at[:, col_span(other, 0)], STEP),
             (feat_src_f32, feat_src, depth), (feat_tgt_f32, feat_tgt, depth)]
    head_loads, head_stores = [], []
    for n, (source, target, size) in enumerate(heads):
        head_loads.append(pltpu.make_async_copy(source, acc.at[:, pl.ds(n * size, size)], load_sem.at[2 + n]))
        head_loads[-1].start()
        head_stores.append(pltpu.make_async_copy(left_buf.at[n // 2, :, pl.ds(n % 2 * size, size)], target, load_sem.at[2 + n]))
    mass_all[me] = mass_mine[...]
    barrier = pltpu.get_barrier_semaphore()
    for peer in peers:
        pl.semaphore_signal(barrier, inc=1, device_id={'rows': peer}, device_id_type=MESH)
    pl.semaphore_wait(barrier, GROUP - 1)

    counter = [0]

    def reserve(count):
        counter[0] += count
        return counter[0] - count

    def remote(source, target, peer, index):
        return pltpu.make_async_remote_copy(src_ref=source, dst_ref=target, send_sem=send_sem.at[index],
                                            recv_sem=recv_sem.at[index], device_id={'rows': peer}, device_id_type=MESH)

    def block_spots():
        diag, off = me * rows, (me + 1 - 2 * core) * rows
        return [(0, diag), (0, diag + quad), (quad, diag + quad), (0, off + quad * core), (quad * core, off + quad)]

    src_near_out = remote(src, src_near, near, reserve(1))
    src_feat_near = remote(feat_src, src_feat_peer.at[0], near, reserve(1))
    start_near_out = remote(start.at[:, aligned(other, half)], start_near, near, reserve(1))
    tgt_near_out = remote(tgt, tgt_near, near, reserve(1))
    tgt_feat_near = remote(feat_tgt, tgt_feat_peer.at[0], near, reserve(1))
    src_out = [remote(src.at[aligned(row, quad), aligned(col, quad)], src_blocks.at[0, b], same, reserve(1))
               for b, (row, col) in enumerate(block_spots())]
    src_feat_out = remote(feat_src, src_feat_peer.at[1], same, reserve(1))
    feat_part = rows // PIECES
    tgt_feat_out = [remote(feat_tgt.at[pl.ds(i * feat_part, feat_part)], tgt_feat_peer.at[1, pl.ds(i * feat_part, feat_part)],
                           same, reserve(1)) for i in range(PIECES)]
    piece = quad // PIECES
    tgt_out = [remote(tgt.at[aligned(row + h * piece, piece), aligned(col, quad)],
                      tgt_blocks.at[0, b, pl.ds(h * piece, piece)], same, reserve(1))
               for b, (row, col) in enumerate(block_spots()) for h in range(PIECES)]
    src_pass = remote(src_blocks.at[0], src_blocks.at[1], near, reserve(1))
    src_feat_pass = remote(src_feat_peer.at[1], src_feat_peer.at[2], near, reserve(1))
    tgt_pass = remote(tgt_blocks.at[0], tgt_blocks.at[1], near, reserve(1))
    tgt_feat_pass = remote(tgt_feat_peer.at[1], tgt_feat_peer.at[2], near, reserve(1))
    mass_out = [remote(mass_mine, mass_all.at[me], peer, reserve(1)) for peer in peers]
    start_base = reserve(2 * steps)
    near_base = reserve(2)
    late_pieces = tgt_out[TAIL_PIECES:] + tgt_feat_out

    def start_out(s):
        return [remote(start.at[:, col_span(mine, s)], start_far.at[0, :, col_span(0, s)], same, start_base + s),
                remote(start.at[:, col_span(other, s)], start_far.at[1, :, col_span(0, s)], cross, start_base + steps + s)]

    def near_copy(slot):
        return remote(own_buf.at[slot], near_buf.at[slot], near, near_base + slot)

    for n, (_, _, size) in enumerate(heads):
        head_loads[n].wait()

        def cast_head(t, carry, n=n, size=size):
            span = aligned(t * 256, 256)
            left_buf[n // 2, span, n % 2 * size:(n % 2 + 1) * size] = acc[span, n * size:(n + 1) * size].astype(BF16)
            return carry
        lax.fori_loop(0, rows // 256, cast_head, 0)
        head_stores[n].start()
    for load in src_load_all:
        load.start()
    for store in head_stores:
        store.wait()
    for copy in start_out(0):
        copy.start()
    for copy in [src_feat_near, tgt_feat_near] + mass_out:
        copy.start()

    src_stores = []
    for b in range(2):
        src_load_all[b].wait()

        def cast(t, carry, b=b):
            span = aligned(t * BLOCK, BLOCK)
            src_buf[b, span, :] = acc[aligned(b * quad + t * BLOCK, BLOCK), :].astype(BF16)
            return carry
        lax.fori_loop(0, quad // BLOCK, cast, 0)
        src_stores.append(pltpu.make_async_copy(src_buf.at[b], src.at[pl.ds(b * quad, quad)], src_sem.at[b, 0]))
        src_stores[-1].start()
    start_load = pltpu.make_async_copy(start_f32, acc, load_sem.at[0])
    start_load.start()
    for store in src_stores:
        store.wait()
    for copy in [src_feat_out, src_near_out] + src_out:
        copy.start()

    def cast_keep(t, carry):
        span = aligned(t * BLOCK, BLOCK)
        keep[span, :] = acc[span, :].astype(BF16)
        return carry
    start_load.wait()
    lax.fori_loop(0, rows // BLOCK, cast_keep, 0)
    tgt_load_all = pltpu.make_async_copy(tgt_f32, acc, load_sem.at[0])
    tgt_load_all.start()
    rest = half - STEP
    start_stores = []
    for n, base in enumerate((mine, other)):
        span = pl.ds(pl.multiple_of(base + STEP, STEP), rest)
        start_stores.append(pltpu.make_async_copy(keep.at[:, span], start.at[:, span], load_sem.at[2 + n]))
        start_stores[-1].start()
    for store in start_stores:
        store.wait()
    for s in range(1, steps):
        for copy in start_out(s):
            copy.start()
    start_near_out.start()
    tgt_load_all.wait()
    lax.fori_loop(0, rows // BLOCK, cast_keep, 0)
    tgt_store = pltpu.make_async_copy(keep, tgt, load_sem.at[0])
    tgt_store.start()
    tgt_store.wait()
    tgt_near_out.start()
    for copy in tgt_out[:TAIL_PIECES]:
        copy.start()

    def cross_terms(first, peer_second):
        depth = feat_buf.shape[1]
        seconds = [left_buf.at[k // 2, :, pl.ds(k % 2 * depth, depth)] for k in range(GROUP)]
        loads = [pltpu.make_async_copy(first, feat_buf, load_sem.at[1])]
        loads += [pltpu.make_async_copy(peer_second(k), seconds[k], load_sem.at[2 + k]) for k in range(GROUP)]
        for load in loads:
            load.start()
        for load in loads:
            load.wait()
        for k, device in enumerate(devices):

            def cross_term(h, carry, device=device, k=k):
                second = left_buf[k // 2, aligned(h * TILE, TILE), k % 2 * depth:(k % 2 + 1) * depth]
                acc[:, aligned(device * rows + h * TILE, TILE)] = weighted(mm(feat_buf[...], second, NT), 2.0 * ALPHA)
                return carry
            lax.fori_loop(0, rows // TILE, cross_term, 0)

    src_near_out.wait_recv()
    turn_corner(src, src_near, src_far, slab, turned, block_sem, chip, core, rows)
    src_feat_near.wait_recv()
    src_feat_out.wait_recv()
    src_feat_pass.start()
    src_feat_pass.wait_recv()
    cross_terms(feat_tgt, lambda k: feat_src if k == 0 else src_feat_peer.at[k - 1])
    tgt_near_out.wait_recv()
    turn_corner(tgt, tgt_near, tgt_far, slab, turned, block_sem, chip, core, rows)
    for copy in src_out:
        copy.wait_recv()
    src_pass.start()
    src_pass.wait_recv()
    place_corner(src_blocks, src_far, slab, turned, block_sem, chip, core, rows)

    def rows_of(matrix, matrix_near, matrix_far, k, h):
        if k == 0:
            return matrix.at[pl.ds(h * SLAB, SLAB)]
        if k == 1:
            return matrix_near.at[pl.ds(h * SLAB, SLAB)]
        which = core if k == 2 else 1 - core
        return matrix_far.at[aligned(which * rows + h * SLAB, SLAB)]

    ordered = [(k, h) for k in range(GROUP) for h in range(per)]

    def src_load(b):
        return Copies(rows_of(src, src_near, src_far, *ordered[b]), src_buf.at[b % 2], src_sem.at[b % 2], SLAB)

    def gather(parts):
        def update(h, carry):
            span = aligned(h * TILE, TILE)
            left = [keep[:, col_span(base, s)] for base, s, _, _ in parts]
            right = [buf[slot, span, :] for _, _, buf, slot in parts]
            block = mm(jnp.concatenate(left, axis=1), jnp.concatenate(right, axis=1), NT)
            acc[:, span] += weighted(block, 2.0 * (1.0 - ALPHA))
            return carry
        lax.fori_loop(0, cols // TILE, update, 0)

    start_near_out.wait_recv()
    src_load(0).start()

    def step(s, carry):
        slot = lax.rem(s, 2)
        for copy in start_out(s):
            copy.wait_recv()
        loads = []
        for k, device in enumerate(devices):
            source = (start.at[:, col_span(mine, s)] if k == 0 else start_near.at[:, col_span(0, s)] if k == 1
                      else start_far.at[k - 2, :, col_span(0, s)])
            landing = turned.at[pl.ds(k // 2 * rows, rows), pl.ds(k % 2 * STEP, STEP)]
            loads.append(pltpu.make_async_copy(source, landing, load_sem.at[2 + k]))
        for load in loads:
            load.start()

        @pl.when(s >= 2)
        def _():
            near_copy(slot).wait_send()
        for k, load in enumerate(loads):
            load.wait()

            def turn(t, carry, k=k):
                block = turned[aligned(k // 2 * rows + t * STEP, STEP), pl.ds(k % 2 * STEP, STEP)]
                start_buf[:, aligned(devices[k] * rows + t * STEP, STEP)] = block.T
                return carry
            lax.fori_loop(0, rows // STEP, turn, 0, unroll=2)
        for b, (k, h) in enumerate(ordered):
            src_load(b).wait()
            if b + 1 < len(ordered):
                src_load(b + 1).start()
            else:
                @pl.when(s + 1 < steps)
                def _():
                    src_load(0).start()

            def part_a(t, carry, b=b, k=k, h=h):
                value = mm(src_buf[b % 2, aligned(t * PART, PART), :], start_buf[...], NT).astype(BF16)
                own_buf[slot, aligned(devices[k] * rows + h * SLAB + t * PART, PART), :] = value
                return carry
            lax.fori_loop(0, SLAB // PART, part_a, 0, unroll=2)

        @pl.when(s >= 2)
        def _():
            pl.semaphore_wait(free_sem, 1)
        near_copy(slot).start()

        @pl.when(s == 0)
        def _():
            gather([(mine, s, own_buf, slot)])

        @pl.when(s >= 1)
        def _():
            near_copy(1 - slot).wait_recv()
            gather([(mine, s, own_buf, slot), (other, s - 1, near_buf, 1 - slot)])

        @pl.when(jnp.logical_and(s >= 1, s - 1 < steps - 2))
        def _():
            pl.semaphore_signal(free_sem, inc=1, device_id={'rows': near}, device_id_type=MESH)
        return carry
    lax.fori_loop(0, steps, step, 0)
    final = (steps - 1) % 2
    near_copy(final).wait_recv()
    gather([(other, steps - 1, near_buf, final)])

    def tile(j, t):
        begin = j * width + t * LANES
        return slice(begin, begin + LANES)

    def sweeps(phase, transposed, mass_row, mass_col, extra):
        def sends(slot, j):
            return [pltpu.make_async_remote_copy(
                src_ref=part_sum.at[phase, slot, j], dst_ref=peer_sum.at[phase, slot, k, j],
                send_sem=sum_send.at[phase, slot, k, j], recv_sem=sum_recv.at[phase, slot, k, j],
                device_id={'rows': peers[k]}, device_id_type=MESH) for k in range(GROUP - 1)]

        def top_sends(j):
            return [pltpu.make_async_remote_copy(
                src_ref=part_top.at[j], dst_ref=peer_top.at[k, j], send_sem=top_send.at[k, j],
                recv_sem=top_recv.at[k, j], device_id={'rows': peers[k]}, device_id_type=MESH) for k in range(GROUP - 1)]

        def row_update():
            for h in range(0, rows, 256):
                span = slice(h, h + 256)
                row_scale[span, :] = mass_row[span, :] / jnp.sum(row_acc[span, :], axis=1, keepdims=True)

        def col_pass(slot, j):
            def body(i, sums):
                span = pl.ds(i * BLOCK, BLOCK)
                scale = split(row_scale[span, :])
                return tuple(sums[t] + jnp.sum(split(acc[span, tile(j, t)]) * scale, axis=0) for t in range(tiles))
            sums = lax.fori_loop(0, rows // BLOCK, body, tuple(jnp.zeros((8, LANES), F32) for _ in range(tiles)), unroll=2)
            total = jnp.concatenate([jnp.sum(s, axis=0, keepdims=True) for s in sums], axis=0)
            if transposed:
                total = total * shift_fix[j]
            part_sum[phase, slot, j] = total
            for send in sends(slot, j):
                send.start()

        def col_update(slot, j):
            for send in sends(slot, j):
                send.wait()
            total = part_sum[phase, slot, j]
            for k in range(GROUP - 1):
                total = total + peer_sum[phase, slot, k, j]
            scale = mass_col[j] / total
            if transposed:
                scale = scale * shift_fix[j]
            col_scale[j] = scale

        def scale_rows(j):
            return [jnp.broadcast_to(col_scale[j, t:t + 1, :], (8, LANES)) for t in range(tiles)]

        def row_pass(j):
            scale = scale_rows(j)

            def body(i, carry):
                span = pl.ds(i * BLOCK, BLOCK)
                total = None if j == 0 else split(row_acc[span, :])
                for t in range(tiles):
                    term = split(acc[span, tile(j, t)]) * scale[t][None]
                    total = term if total is None else total + term
                row_acc[span, :] = total.reshape(BLOCK, LANES)
                return carry
            lax.fori_loop(0, rows // BLOCK, body, 0, unroll=2)

        if transposed:
            for j in range(CHUNKS):
                def top_block(i, tops, j=j):
                    span = pl.ds(i * BLOCK, BLOCK)
                    return tuple(jnp.maximum(tops[t], jnp.max(split(acc[span, tile(j, t)]), axis=0)) for t in range(tiles))
                tops = lax.fori_loop(0, rows // BLOCK, top_block, tuple(acc[0:8, tile(j, t)] for t in range(tiles)))
                tops = [jnp.max(top, axis=0, keepdims=True) for top in tops]
                wide = [jnp.broadcast_to(top, (8, LANES)) for top in tops]

                def exp_block(i, sums, j=j, wide=wide):
                    span = pl.ds(i * BLOCK, BLOCK)
                    out = []
                    for t in range(tiles):
                        val = jnp.exp((split(acc[span, tile(j, t)]) - wide[t][None]) * inv_eps)
                        acc[span, tile(j, t)] = val.reshape(BLOCK, LANES)
                        out.append(sums[t] + jnp.sum(val, axis=0))
                    return tuple(out)
                sums = lax.fori_loop(0, rows // BLOCK, exp_block, tuple(jnp.zeros((8, LANES), F32) for _ in range(tiles)))
                part_top[j, 0] = jnp.concatenate(tops, axis=0)
                part_top[j, 1] = jnp.concatenate([jnp.sum(s, axis=0, keepdims=True) for s in sums], axis=0)
                for send in top_sends(j):
                    send.start()
            for j in range(CHUNKS):
                for send in top_sends(j):
                    send.wait()
                top = part_top[j, 0]
                for k in range(GROUP - 1):
                    top = jnp.maximum(top, peer_top[k, j, 0])
                fix = jnp.exp((part_top[j, 0] - top) * inv_eps)
                total = part_top[j, 1] * fix
                for k in range(GROUP - 1):
                    total = total + peer_top[k, j, 1] * jnp.exp((peer_top[k, j, 0] - top) * inv_eps)
                shift_fix[j] = fix
                col_scale[j] = mass_col[j] / total * fix
                row_pass(j)
        else:
            def exp_rows(i, carry):
                span = pl.ds(i * BLOCK, BLOCK)
                top = acc[span, 0:LANES]
                for t in range(1, cols // LANES):
                    top = jnp.maximum(top, acc[span, t * LANES:(t + 1) * LANES])
                top = jnp.max(top, axis=1, keepdims=True)
                total = jnp.zeros((BLOCK, LANES), F32)
                for t in range(cols // LANES):
                    val = jnp.exp((acc[span, t * LANES:(t + 1) * LANES] - top) * inv_eps)
                    acc[span, t * LANES:(t + 1) * LANES] = val
                    total = total + val
                row_acc[span, :] = total
                return carry
            lax.fori_loop(0, rows // BLOCK, exp_rows, 0)
        row_update()

        def sweep(n, carry):
            slot = lax.rem(n, 2)
            for j in range(CHUNKS):
                col_pass(slot, j)
            extra(n)
            for j in range(CHUNKS):
                col_update(slot, j)
                row_pass(j)
            row_update()
            return carry
        if not transposed:
            extra(0)
        lax.fori_loop(0, SWEEPS - 1, sweep, 0)
        if transposed:
            for j in range(CHUNKS):
                scale = scale_rows(j)

                def plan_block(i, carry, j=j, scale=scale):
                    span = pl.ds(i * BLOCK, BLOCK)
                    left = split(row_scale[span, :])
                    for t in range(tiles):
                        val = left * split(acc[span, tile(j, t)]) * scale[t][None]
                        keep[span, tile(j, t)] = val.reshape(BLOCK, LANES).astype(BF16)
                    return carry
                lax.fori_loop(0, rows // BLOCK, plan_block, 0)
        else:
            for j in range(CHUNKS):
                col_pass((SWEEPS - 1) % 2, j)
            for j in range(CHUNKS):
                col_update((SWEEPS - 1) % 2, j)

    def late(n):
        for index, copy in enumerate(late_pieces):
            pl.when(n == index)(copy.start)

    for copy in mass_out:
        copy.wait_recv()
    sweeps(0, True, mass_rows_t, mass_all, late)

    order = [(k, h) for k in (2, 3, 1, 0) for h in range(per)]

    def src_again(n):
        return Copies(rows_of(src, src_near, src_far, *order[n]), src_buf.at[n % 2], src_sem.at[n % 2], SLAB)

    column = aligned(me * rows, rows)
    a_copies, own_stores = [], []
    src_again(0).start()
    for n, (k, h) in enumerate(order):
        src_again(n).wait()
        if n + 1 < len(order):
            src_again(n + 1).start()

        def make(t, carry, n=n):
            span = aligned(t * 256, 256)
            made[n, :, span] = mm(src_buf[n % 2], keep[span, :], NT).astype(BF16)
            return carry
        lax.fori_loop(0, rows // 256, make, 0, unroll=2)
        target = ready.at[pl.ds(h * SLAB, SLAB), column]
        if k:
            a_copies.append(remote(made.at[n], target, devices[k], reserve(1)))
            a_copies[-1].start()
        else:
            own_stores.append(pltpu.make_async_copy(made.at[n], target, block_sem.at[h]))
            own_stores[-1].start()

    tgt_feat_near.wait_recv()
    for copy in tgt_feat_out:
        copy.wait_recv()
    tgt_feat_pass.start()
    for copy in tgt_out:
        copy.wait_recv()
    tgt_pass.start()
    tgt_feat_pass.wait_recv()
    cross_terms(feat_src, lambda k: feat_tgt if k == 0 else tgt_feat_peer.at[k - 1])
    tgt_pass.wait_recv()
    for store in own_stores:
        store.wait()
    place_corner(tgt_blocks, tgt_far, slab, turned, block_sem, chip, core, rows)

    def stage(k):
        if k % 2 == 0:
            return [src_buf.at[h] for h in range(per)], [left_buf.at[h] for h in range(per)]
        return [keep.at[pl.ds(h * SLAB, SLAB)] for h in range(per)], [turned.at[pl.ds(h * rows, rows)] for h in range(per)]

    def tgt_loads(k):
        return [Copies(rows_of(tgt, tgt_near, tgt_far, k, h), stage(k)[0][h], src_sem.at[k % 2 * per + h], SLAB)
                for h in range(per)]

    def left_loads(k):
        return [pltpu.make_async_copy(ready.at[:, aligned(devices[k] * rows + h * SLAB, SLAB)], stage(k)[1][h],
                                      load_sem.at[k % 2 * per + h]) for h in range(per)]

    def half_loads(part):
        k = GROUP - 1
        return [pltpu.make_async_copy(
            ready.at[pl.ds(part * SLAB, SLAB), aligned(devices[k] * rows + h * SLAB, SLAB)],
            stage(k)[1][h].at[pl.ds(part * SLAB, SLAB)], load_sem.at[k % 2 * per + h]) for h in range(per)]

    def begin_left(k):
        for copy, (kk, _) in zip(a_copies, order):
            if kk == k:
                copy.wait_recv()
        for load in left_loads(k):
            load.start()

    for load in tgt_loads(0):
        load.start()
    begin_left(0)
    for k in range(GROUP):
        if k + 1 < GROUP:
            for load in tgt_loads(k + 1):
                load.start()
        if k == GROUP - 1:
            break
        if k + 1 < GROUP - 1:
            begin_left(k + 1)
        for load in tgt_loads(k) + left_loads(k):
            load.wait()
        rights, lefts = stage(k)

        def update(t, carry, rights=rights, lefts=lefts):
            span = aligned(t * STEP, STEP)
            total = mm(lefts[0][...], rights[0][:, span], NN)
            for h in range(1, per):
                total = total + mm(lefts[h][...], rights[h][:, span], NN)
            acc[:, span] += weighted(total, 2.0 * (1.0 - ALPHA))
            return carry
        lax.fori_loop(0, cols // STEP, update, 0)

    for load in tgt_loads(GROUP - 1):
        load.wait()
    rights, lefts = stage(GROUP - 1)
    for part in range(per):
        for copy, spot in zip(a_copies, order):
            if spot == (GROUP - 1, part):
                copy.wait_recv()
        for load in half_loads(part):
            load.start()
        for load in half_loads(part):
            load.wait()
        row_span = pl.ds(part * SLAB, SLAB)

        def update_half(t, carry, row_span=row_span):
            span = aligned(t * TILE, TILE)
            total = mm(lefts[0][row_span, :], rights[0][:, span], NN)
            for h in range(1, per):
                total = total + mm(lefts[h][row_span, :], rights[h][:, span], NN)
            acc[row_span, span] += weighted(total, 2.0 * (1.0 - ALPHA))
            return carry
        lax.fori_loop(0, cols // TILE, update_half, 0)

    kern_store = pltpu.make_async_copy(acc, kern_out, load_sem.at[2])

    def store_kernel(n):
        if isinstance(n, int):
            kern_store.start()
    sweeps(1, False, mass_rows, mass_cols, store_kernel)
    row_out[...] = row_scale[...]
    col_out[...] = col_scale[...]
    kern_store.wait()
    for slot in range(2):
        near_copy(slot).wait_send()
    for copy in ([src_near_out, src_feat_near, start_near_out, tgt_near_out, tgt_feat_near, src_feat_out,
                  src_pass, src_feat_pass, tgt_pass, tgt_feat_pass] + src_out + tgt_out + tgt_feat_out + mass_out + a_copies):
        copy.wait_send()
    for s in range(steps):
        for copy in start_out(s):
            copy.wait_send()


def solution(mesh):
    def local_fgw(cost_src, cost_tgt, plan_init, mass_src, mass_tgt, feat_src, feat_tgt, epsilon):
        rows, cols = cost_src.shape
        half, quad = cols // 2, rows // 2
        depth = feat_src.shape[1]
        tiles = cols // LANES // CHUNKS
        me = lax.axis_index('rows')
        mass_cols_mine = lax.dynamic_slice(mass_tgt, (rows * me,), (rows,))
        vec = (CHUNKS, tiles, LANES)
        n_links = 44 + 2 * (half // STEP) + 2 + 3 * rows // SLAB
        any_spec = pl.BlockSpec(memory_space=pl.ANY)
        vmem_spec = pl.BlockSpec(memory_space=pltpu.VMEM)
        hbm = [((rows, cols), BF16), ((rows, depth), BF16), ((rows, depth), BF16),
               ((rows, cols), BF16), ((rows, cols), BF16),
               ((rows, cols), BF16), ((2, 5, quad, quad), BF16), ((half, cols), BF16),
               ((rows, cols), BF16), ((2, 5, quad, quad), BF16), ((half, cols), BF16),
               ((GROUP - 1, rows, depth), BF16), ((GROUP - 1, rows, depth), BF16),
               ((rows, half), BF16), ((2, rows, half), BF16), ((rows, cols), BF16)]
        outs = [((rows, cols), F32), ((rows, LANES), F32), (vec, F32)] + hbm
        vmem = [((rows, cols), F32), ((rows, cols), BF16), ((2, SLAB, cols), BF16), ((STEP, cols), BF16),
                ((2, cols, STEP), BF16), ((2, cols, STEP), BF16), ((GROUP * rows // SLAB, SLAB, rows), BF16),
                ((2, rows, SLAB), BF16), ((SLAB, half), BF16), ((half, SLAB), BF16), ((rows, depth), BF16),
                (vec, F32), ((rows, LANES), F32), ((rows, LANES), F32), (vec, F32), (vec, F32),
                ((2, 2) + vec, F32), ((2, 2, GROUP - 1) + vec, F32),
                ((CHUNKS, 2, tiles, LANES), F32), ((GROUP - 1, CHUNKS, 2, tiles, LANES), F32)]
        sems = [(8,), (4, SPLIT), (15,), (n_links,), (n_links,), (2, 2, GROUP - 1, CHUNKS), (2, 2, GROUP - 1, CHUNKS),
                (GROUP - 1, CHUNKS), (GROUP - 1, CHUNKS)]
        result = pl.pallas_call(
            kernel,
            out_shape=[jax.ShapeDtypeStruct(*s) for s in outs],
            in_specs=[any_spec] * 5 + [vmem_spec] * 4 + [pl.BlockSpec(memory_space=pltpu.SMEM)],
            out_specs=[any_spec, vmem_spec, vmem_spec] + [any_spec] * len(hbm),
            scratch_shapes=[pltpu.VMEM(*s) for s in vmem] + [pltpu.SemaphoreType.DMA(s) for s in sems]
            + [pltpu.SemaphoreType.REGULAR],
            compiler_params=pltpu.CompilerParams(collective_id=0, has_side_effects=True, vmem_limit_bytes=67000000),
            cost_estimate=pl.CostEstimate(flops=10 * rows * cols * cols, bytes_accessed=700000000,
                                          transcendentals=2 * rows * cols),
            name='fused_gw',
        )(cost_src, cost_tgt, plan_init, feat_src, feat_tgt,
          mass_src.reshape(tiles, LANES), jnp.broadcast_to(mass_cols_mine[:, None], (rows, LANES)),
          jnp.broadcast_to(mass_src[:, None], (rows, LANES)), mass_tgt.reshape(vec), epsilon.reshape(1))
        kern, row_scale, col_scale = result[:3]
        return row_scale[:, :1] * kern * col_scale.reshape(1, cols)

    row_spec = P(('pairs', 'rows'), None)
    vec_spec = P(('pairs', 'rows'))
    in_specs = (row_spec, row_spec, row_spec, vec_spec, P('pairs'), row_spec, row_spec, P())
    return jax.shard_map(local_fgw, mesh=mesh, in_specs=in_specs, out_specs=row_spec, check_vma=False)
```
